256 devices in a mesh: dp: 8 (over z), expert: 16 (over y, x), tensor: 2 (over core).
Axes of the slice: x: 4, y: 4, z: 8, core: 2. Of those that a mesh axis runs over, the one named last changes fastest.
Arguments:
- tokens: bfloat16 [1536, 7168], P(('dp', 'expert')), may hold values from -6 to 6
- expert_ids: int32 [1536, 8], P(('dp', 'expert')), may hold values from 0 to 15, all different within a row; in each aligned block of 12 rows (0 to 11, 12 to 23, ...) at most 8 rows name the same one
- route_weights: float32 [1536, 8], P(('dp', 'expert')), may hold values from 0.1 to 1
- gate_weights: bfloat16 [16, 7168, 2048], P('expert', 'dp', 'tensor'), may hold values from -0.0625 to 0.0625
- up_weights: bfloat16 [16, 7168, 2048], P('expert', 'dp', 'tensor'), may hold values from -0.0625 to 0.0625
- down_weights: bfloat16 [16, 2048, 7168], P('expert', 'tensor', 'dp'), may hold values from -0.125 to 0.125
- shared_gate: bfloat16 [7168, 2048], P('dp', 'tensor'), may hold values from -0.0625 to 0.0625
- shared_up: bfloat16 [7168, 2048], P('dp', 'tensor'), may hold values from -0.0625 to 0.0625
- shared_down: bfloat16 [2048, 7168], P('tensor', 'dp'), may hold values from -0.125 to 0.125
Outputs:
- mixed: bfloat16 [1536, 7168], P(('dp', 'expert'))
The draws below stay inside these ranges and needn't reach their ends.
Inputs may be any that keep to these rules, and one draw needn't show every extreme that they name: `expert_ids`: each token names 8 different experts. In the rows of one device no expert is named by more than 8 tokens, and in some device's rows some expert is named by exactly 8.
All inputs are finite; a program needn't handle non-finite values.
Results may differ from the reference program's by a relative error of at most 0.005.
Values may be sent and summed in bfloat16 or wider, within the bound.
No kernel may reach another device: no remote copies, remote signals or barrier semaphores. Data moves between devices by JAX's collectives and lax.ppermute only.
A program may use at most 128 MiB of HBM per device.

```python
import math
import jax
import jax.numpy as jnp
import numpy as np
from jax import lax

D = 7168
FF = 2048
TOP = 8
EXPERTS = 16
TOK_DEV = 12
CAP = 8
TOKENS = 1536


def block_levels(own_key, shape, shards, smallest, high):
    gain, own = 1.0, jax.random.fold_in(own_key, 6)
    for axis_at, shards_of in shards:
        heights = jnp.exp(jax.random.uniform(jax.random.fold_in(own, axis_at), (shards_of,), jnp.float32, smallest / len(shards), high / len(shards)))
        gain = gain * jnp.repeat(heights, shape[axis_at] // shards_of).reshape([-1 if axis == axis_at else 1 for axis in range(len(shape))])
    return gain


def assign_block(stream_key, own, number, rows, amount, top, limit, skew):
    sequence = jax.random.permutation(stream_key, amount)
    packed, common = shares(amount, rows * top, limit, skew, True), shares(amount, rows * top, limit, skew, False)
    places = jnp.arange(amount)

    def named(lengths, offset_by):
        used = int((lengths > 0).sum())
        fixed = max(1, used // 4)
        passed = fixed + (places - fixed + offset_by * (used - fixed)) % max(1, amount - fixed)
        return jnp.zeros((amount,), jnp.int32).at[sequence[jnp.where(places < fixed, places, passed)]].set(jnp.asarray(lengths, jnp.int32))

    lengths = jnp.where(number % 4 == 0, named(packed, number // 4), named(common, number - number // 4 - 1))
    mixed = jax.random.permutation(jax.random.fold_in(own, 3), amount)
    donor, sink = mixed[0:amount // 2 * 2:2], mixed[1:amount // 2 * 2:2]
    margin = jnp.minimum(lengths[donor] - 1, limit - lengths[sink]) // 2
    margin = jnp.where((donor == sequence[0]) | (sink == sequence[0]) | (lengths[sink] == 0), 0, jnp.maximum(margin, 0))
    passed = jax.random.randint(jax.random.fold_in(own, 4), (amount // 2,), 0, 1 << 20) % (margin + 1)
    lengths = lengths.at[donor].add(-passed).at[sink].add(passed)
    labels = jnp.searchsorted(jnp.cumsum(lengths), jnp.arange(rows * top), side="right").astype(jnp.int32)
    table = labels.reshape(top, rows).T
    table = table[jax.random.permutation(jax.random.fold_in(own, 1), rows)]
    offset_by = jax.random.randint(jax.random.fold_in(own, 2), (rows, 1), 0, top)
    return jnp.take_along_axis(table, (jnp.arange(top)[None, :] + offset_by) % top, axis=1)


def shares(number_of, total, limit, lean, full):
    loads = [(1 << 20) // math.isqrt(grade ** lean) + 1 for grade in range(1, number_of + 1)]
    largest = limit if full else min(limit, max(-(-total // number_of), total * loads[0] // sum(loads)))
    least = 1 if total - largest >= number_of - 1 else 0
    counts, spare = [largest] + [least] * (number_of - 1), total - largest - least * (number_of - 1)
    while spare > 0:
        movable = [i for i in range(1, number_of) if counts[i] < largest] or [i for i in range(1, number_of) if counts[i] < limit]
        mass, remaining = sum([loads[i] for i in movable]), spare
        for i in movable:
            addition = min(limit - counts[i], max(1, remaining * loads[i] // mass), spare)
            counts[i] = counts[i] + addition
            spare = spare - addition
    return np.array(counts)


def noise(key, shape, width, limit, cuts=(), kind=jnp.bfloat16):
    gain = block_levels(key, shape, cuts, -0.22, 0.18) if cuts else 1.0
    array = jax.random.normal(key, shape, jnp.float32) * width * gain
    return jnp.minimum(jnp.maximum(array, -limit), limit).astype(kind)


def setup_inputs(seed: int = 0) -> dict:
    key_of = jax.random.split(jax.random.key(seed), 10)
    tokens = noise(key_of[0], (TOKENS, D), 1.0, 6.0, ((0, 128),))
    expert_ids_keys = jax.random.split(jax.random.fold_in(key_of[1], 1), TOKENS // TOK_DEV)
    expert_ids_turns = jax.random.permutation(jax.random.fold_in(key_of[1], 3), TOKENS // TOK_DEV)
    expert_ids = jax.vmap(lambda own, number: assign_block(jax.random.fold_in(key_of[1], 2), own, number, TOK_DEV, EXPERTS, TOP, CAP, 2))(expert_ids_keys, expert_ids_turns).reshape((TOKENS, TOP))
    route_weights = jnp.clip(jnp.exp(math.log(1.0) - 2.3025851 * jax.random.uniform(key_of[2], (TOKENS, TOP), jnp.float32) ** block_levels(key_of[2], (TOKENS, TOP), ((0, 128),), -0.2, 0.2)), 0.1, 1.0)
    gate_weights = noise(key_of[3], (EXPERTS, D, FF), D ** -0.5, 0.0625, ((0, 16), (1, 8), (2, 2)))
    up_weights = noise(key_of[4], (EXPERTS, D, FF), D ** -0.5, 0.0625, ((0, 16), (1, 8), (2, 2)))
    down_weights = noise(key_of[5], (EXPERTS, FF, D), FF ** -0.5, 0.125, ((0, 16), (1, 2), (2, 8)))
    shared_gate = noise(key_of[6], (D, FF), D ** -0.5, 0.0625, ((0, 8), (1, 2)))
    shared_up = noise(key_of[7], (D, FF), D ** -0.5, 0.0625, ((0, 8), (1, 2)))
    shared_down = noise(key_of[8], (FF, D), FF ** -0.5, 0.125, ((0, 2), (1, 8)))
    return dict(tokens=tokens, expert_ids=expert_ids, route_weights=route_weights, gate_weights=gate_weights, up_weights=up_weights, down_weights=down_weights, shared_gate=shared_gate, shared_up=shared_up, shared_down=shared_down)


def reference(tokens, expert_ids, route_weights, gate_weights, up_weights, down_weights, shared_gate, shared_up, shared_down):
    shared_gate_out = jnp.dot(tokens, shared_gate, preferred_element_type=jnp.float32)
    shared_up_out = jnp.dot(tokens, shared_up, preferred_element_type=jnp.float32)
    shared_hidden = (jax.nn.silu(shared_gate_out) * shared_up_out).astype(jnp.bfloat16)
    shared_out = jnp.dot(shared_hidden, shared_down, preferred_element_type=jnp.float32)

    def accumulate(running, layer_pack):
        gate_matrix, up_matrix, down_matrix, expert_index = layer_pack
        gate_out = jnp.dot(tokens, gate_matrix, preferred_element_type=jnp.float32)
        up_out = jnp.dot(tokens, up_matrix, preferred_element_type=jnp.float32)
        hidden = (jax.nn.silu(gate_out) * up_out).astype(jnp.bfloat16)
        expert_out = jnp.dot(hidden, down_matrix, preferred_element_type=jnp.float32)
        coefficient = jnp.sum(jnp.where(expert_ids == expert_index, route_weights, jnp.zeros_like(route_weights)), axis=1)
        return running + coefficient[:, None] * expert_out.astype(running.dtype), None

    indices = jnp.arange(EXPERTS, dtype=jnp.int32)
    running, unused = lax.scan(accumulate, shared_out, (gate_weights, up_weights, down_weights, indices))
    return running.astype(jnp.bfloat16)
```

```python
import functools

import jax
import jax.numpy as jnp
from jax import lax
from jax.experimental import pallas as pl
from jax.experimental.pallas import tpu as pltpu
from jax.sharding import PartitionSpec as P

EXPERTS = 16
CAP = 8
TOP = 8
ZN = 8
TOK = 12
PADT = 16
BLOCK = 896
HALF = 448
WIDE = 512
ROWS = EXPERTS * CAP
CHUNK = ROWS + PADT
FFH = 1024
NT = 256
ORDER = (3, 4, 5, 6, 7, 0, 1, 2)
SCALE = 16.0
LINK = jnp.float16

PARAMS = pltpu.CompilerParams(vmem_limit_bytes=24 * 1024 * 1024)
VMEM = pl.BlockSpec(memory_space=pltpu.VMEM)
SMEM = pl.BlockSpec(memory_space=pltpu.SMEM)
SWAP = [(0, 1), (1, 0)]


def shifted(k):
    return [(i, (i + k) % ZN) for i in range(ZN)]


def paired(up, down):
    out = []
    for i in range(ZN):
        out.append((i * 2, ((i + up) % ZN) * 2))
        out.append((i * 2 + 1, ((i - down) % ZN) * 2 + 1))
    return out


def fdot(a, b):
    return jnp.dot(a, b, preferred_element_type=jnp.float32)


def prep_kernel(c_ref, x_ref, ids_ref, w_ref, out_ref):
    first = c_ref[0] == 0
    w = w_ref[...]
    hi = w.astype(jnp.bfloat16)
    rest = w - hi.astype(jnp.float32)
    mid = rest.astype(jnp.bfloat16)
    low = (rest - mid.astype(jnp.float32)).astype(jnp.bfloat16)
    lane = lax.broadcasted_iota(jnp.int32, (TOP, 128), 1)
    part = lax.broadcasted_iota(jnp.int32, (TOP, 128), 0)
    start = jnp.where(first, 64, 0)
    ext = jnp.zeros((TOK, 128), jnp.float32)
    for i, v in enumerate((ids_ref[...].astype(jnp.float32).astype(jnp.bfloat16), hi, mid, low)):
        ext = ext + fdot(v, (lane == start + TOP * i + part).astype(jnp.bfloat16))
    lanes = lax.broadcasted_iota(jnp.int32, (TOK, 128), 1)
    routing = lanes // 64 == jnp.where(first, 1, 0)
    for b in range(ZN):
        at = b * BLOCK

        @pl.when(first)
        def _():
            out_ref[b, :, :384] = x_ref[:, at : at + 384]
            edge = x_ref[:, at + 384 : at + 512].astype(jnp.float32)
            out_ref[b, :, 384:] = jnp.where(routing, ext, edge).astype(jnp.bfloat16)

        @pl.when(jnp.logical_not(first))
        def _():
            edge = x_ref[:, at + 384 : at + 512].astype(jnp.float32)
            out_ref[b, :, :128] = jnp.where(routing, ext, edge).astype(jnp.bfloat16)
            out_ref[b, :, 128:] = x_ref[:, at + 512 : at + BLOCK]


def prep(c, x, ids, w):
    return pl.pallas_call(
        prep_kernel,
        out_shape=jax.ShapeDtypeStruct((ZN, TOK, WIDE), jnp.bfloat16),
        in_specs=[SMEM, VMEM, VMEM, VMEM],
        out_specs=VMEM,
        compiler_params=PARAMS,
        name="prep",
    )(c, x, ids, w)


def pack_kernel(s_ref, x_ref, packed_ref, shared_ref, ext_ref):
    z = s_ref[0]
    n = ZN * TOK
    x = x_ref[...].astype(jnp.float32)
    x = jnp.where(s_ref[1] == 0, x, pltpu.roll(x, WIDE - 64, 1))
    ext = x[:, WIDE - 128 :]
    ext_ref[...] = ext.astype(jnp.bfloat16)
    x = x.astype(jnp.bfloat16)[:, :HALF]
    ids = jnp.transpose(ext)[64:72, :].astype(jnp.int32)
    experts = lax.broadcasted_iota(jnp.int32, (EXPERTS, n), 0)
    member = jnp.zeros((EXPERTS, n), jnp.float32)
    for k in range(TOP):
        member = member + (experts == ids[k : k + 1, :]).astype(jnp.float32)
    r0 = lax.broadcasted_iota(jnp.int32, (n, n), 0)
    r1 = lax.broadcasted_iota(jnp.int32, (n, n), 1)
    before = ((r0 // TOK == r1 // TOK) & (r0 < r1)).astype(jnp.bfloat16)
    pos = fdot(member.astype(jnp.bfloat16), before).astype(jnp.int32)
    row = lax.broadcasted_iota(jnp.int32, (1, n), 1)
    zs = row // TOK
    place = (z - zs + 13) % ZN
    target = jnp.where(member > 0.5, place * CAP + pos, -1)
    wanted = lax.broadcasted_iota(jnp.int32, (ZN * CAP, n), 0)
    for e in range(EXPERTS):
        pick = (wanted == target[e : e + 1, :]).astype(jnp.bfloat16)
        packed_ref[e] = fdot(pick, x).astype(jnp.bfloat16)
    wide = lax.broadcasted_iota(jnp.int32, (ZN * PADT, n), 0)
    pick = (wide == place * PADT + row - zs * TOK).astype(jnp.bfloat16)
    shared_ref[...] = fdot(pick, x).astype(jnp.bfloat16)


def pack(s, x):
    return pl.pallas_call(
        pack_kernel,
        out_shape=(
            jax.ShapeDtypeStruct((EXPERTS, ZN * CAP, HALF), jnp.bfloat16),
            jax.ShapeDtypeStruct((ZN * PADT, HALF), jnp.bfloat16),
            jax.ShapeDtypeStruct((ZN * TOK, 128), jnp.bfloat16),
        ),
        in_specs=[SMEM, VMEM],
        out_specs=(VMEM, VMEM, VMEM),
        compiler_params=PARAMS,
        name="pack",
    )(s, x)


def up_kernel(first, count, c_ref, own_ref, oth_ref, so_ref, st_ref, wg_ref, wu_ref, sg_ref, su_ref, *out_refs):
    c = c_ref[0]
    mine = pl.ds(pl.multiple_of(c * HALF, 64), HALF)
    other = pl.ds(pl.multiple_of((1 - c) * HALF, 64), HALF)
    own = own_ref[first : first + count].reshape(count * ROWS, HALF)
    oth = oth_ref[first : first + count].reshape(count * ROWS, HALF)
    so = so_ref[first * PADT : (first + count) * PADT]
    st = st_ref[first * PADT : (first + count) * PADT]
    for w_ref, s_ref, o_refs in ((wg_ref, sg_ref, out_refs[:count]), (wu_ref, su_ref, out_refs[count:])):
        full = (fdot(own, w_ref[0, mine, :]) + fdot(oth, w_ref[0, other, :])) * SCALE
        shared = (fdot(so, s_ref[mine, :]) + fdot(st, s_ref[other, :])) * SCALE
        for i in range(count):
            o_refs[i][:ROWS, :] = full[i * ROWS : (i + 1) * ROWS]
            o_refs[i][ROWS:, :] = shared[i * PADT : (i + 1) * PADT]


def up_dots(first, count, c, own, oth, so, st, wg, wu, sg, su):
    whole = lambda *shape: pl.BlockSpec(shape, lambda n: (0,) * len(shape))
    return pl.pallas_call(
        functools.partial(up_kernel, first, count),
        grid=(FFH // NT,),
        out_shape=(jax.ShapeDtypeStruct((CHUNK, FFH), jnp.float32),) * (2 * count),
        in_specs=[
            SMEM,
            whole(ZN, ROWS, HALF),
            whole(ZN, ROWS, HALF),
            whole(ZN * PADT, HALF),
            whole(ZN * PADT, HALF),
            pl.BlockSpec((1, BLOCK, NT), lambda n: (0, 0, n)),
            pl.BlockSpec((1, BLOCK, NT), lambda n: (0, 0, n)),
            pl.BlockSpec((BLOCK, NT), lambda n: (0, n)),
            pl.BlockSpec((BLOCK, NT), lambda n: (0, n)),
        ],
        out_specs=(pl.BlockSpec((CHUNK, NT), lambda n: (0, n)),) * (2 * count),
        compiler_params=PARAMS,
        cost_estimate=pl.CostEstimate(
            flops=2 * 2 * count * CHUNK * BLOCK * FFH, bytes_accessed=4 * BLOCK * FFH * 2, transcendentals=0
        ),
    )(c, own, oth, so, st, wg, wu, sg, su)


def down_kernel(c_ref, *refs):
    xs, (wd_ref, sd_ref, keep_ref, send_ref) = refs[:-4], refs[-4:]
    n = len(xs) // 2
    full = fdot(jnp.concatenate([x[:ROWS] for x in xs], axis=0), wd_ref[0])
    shared = fdot(jnp.concatenate([x[ROWS:] for x in xs], axis=0), sd_ref[...])

    def store(ref, i, at):
        ref[i, :ROWS] = full[at * ROWS : (at + 1) * ROWS]
        ref[i, ROWS:] = shared[at * PADT : (at + 1) * PADT]

    @pl.when(c_ref[0] == 0)
    def _():
        for i in range(n):
            store(keep_ref, i, i)
            store(send_ref, i, n + i)

    @pl.when(c_ref[0] != 0)
    def _():
        for i in range(n):
            store(keep_ref, i, n + i)
            store(send_ref, i, i)


def down_dots(c, xs, wd, sd):
    n = len(xs) // 2
    return pl.pallas_call(
        down_kernel,
        out_shape=(
            jax.ShapeDtypeStruct((n, CHUNK, BLOCK), jnp.float32),
            jax.ShapeDtypeStruct((n, CHUNK, BLOCK), jnp.float32),
        ),
        in_specs=[SMEM] + [VMEM] * (len(xs) + 2),
        out_specs=(VMEM, VMEM),
        compiler_params=PARAMS,
        cost_estimate=pl.CostEstimate(
            flops=2 * 2 * n * CHUNK * BLOCK * FFH, bytes_accessed=2 * BLOCK * FFH * 2, transcendentals=0
        ),
        name="down_dots",
    )(c, *xs, wd, sd)


def combine_kernel(zs_ref, ext_ref, back_ref, shared_ref, out_ref):
    n = ZN * TOK
    rows = 2 * PADT
    cols = 2 * ROWS
    t = lax.broadcasted_iota(jnp.int32, (rows, n), 0)
    r = lax.broadcasted_iota(jnp.int32, (rows, n), 1)
    zs = jnp.where(t < PADT, zs_ref[0], zs_ref[1])
    pick = ((r == zs * TOK + t % PADT) & (t % PADT < TOK)).astype(jnp.bfloat16)
    ext = fdot(pick, ext_ref[...])
    weight = (ext[:, 72:80] + ext[:, 80:88]) + ext[:, 88:96]
    column = lax.broadcasted_iota(jnp.int32, (rows, cols), 1)
    row = lax.broadcasted_iota(jnp.int32, (rows, cols), 0)
    live = (row % PADT < TOK) & (row // PADT == (column // CAP) % 2)
    owner = (column // (2 * CAP)).astype(jnp.float32)
    slot = (column % CAP).astype(jnp.float32)
    member = jnp.zeros((rows, cols), jnp.float32)
    scale = jnp.zeros((rows, cols), jnp.float32)
    for k in range(TOP):
        hit = (ext[:, 64 + k : 65 + k] == owner) & live
        member = jnp.where(hit, 1.0, member)
        scale = jnp.where(hit, weight[:, k : k + 1], scale)
    i0 = lax.broadcasted_iota(jnp.int32, (rows, rows), 0)
    i1 = lax.broadcasted_iota(jnp.int32, (rows, rows), 1)
    before = ((i1 < i0) & (i0 // PADT == i1 // PADT)).astype(jnp.bfloat16)
    pos = fdot(before, member.astype(jnp.bfloat16))
    scale = jnp.where((pos == slot) & (member > 0.5), scale, 0.0)
    hi = scale.astype(jnp.bfloat16)
    rest = scale - hi.astype(jnp.float32)
    mid = rest.astype(jnp.bfloat16)
    low = (rest - mid.astype(jnp.float32)).astype(jnp.bfloat16)
    back = back_ref[...]
    total = (fdot(low, back) + fdot(mid, back)) + fdot(hi, back)
    out_ref[...] = (shared_ref[...] + total).astype(jnp.bfloat16)


def combine(zs, ext, back, shared):
    return pl.pallas_call(
        combine_kernel,
        out_shape=jax.ShapeDtypeStruct((2 * PADT, BLOCK), jnp.bfloat16),
        in_specs=[SMEM, VMEM, VMEM, VMEM],
        out_specs=VMEM,
        compiler_params=PARAMS,
        name="combine",
    )(zs, ext, back, shared)


def assemble_kernel(s_ref, *refs):
    out_ref = refs[-1]
    z = s_ref[0]
    a1, a2, b3, b0, o1, o2, o3, o0 = refs[:-1]

    def put(parts):
        for i, ref in enumerate(parts):
            at = pl.multiple_of(((z + i) % ZN) * BLOCK, 128)
            out_ref[:, pl.ds(at, BLOCK)] = ref[:TOK]

    @pl.when(s_ref[1] == 0)
    def _():
        put((b0, o1, o2, o3, o0, b3, a2, a1))

    @pl.when(s_ref[1] != 0)
    def _():
        put((o0, a1, a2, b3, b0, o3, o2, o1))


def assemble(s, *parts):
    return pl.pallas_call(
        assemble_kernel,
        out_shape=jax.ShapeDtypeStruct((TOK, ZN * BLOCK), jnp.bfloat16),
        in_specs=[SMEM] + [VMEM] * len(parts),
        out_specs=VMEM,
        compiler_params=PARAMS,
        name="assemble",
    )(s, *parts)


def ring(parts, shift):
    total = None
    for mine in parts:
        total = mine if total is None else mine + total.astype(jnp.float32)
        total = lax.ppermute(total.astype(LINK), "dp", shifted(shift))
    return total.astype(jnp.float32)


def layer(tokens, ids, weights, wg, wu, wd, sg, su, sd):
    z = lax.axis_index("dp")
    c = lax.axis_index("tensor")
    c1, zc = c.reshape(1), jnp.stack([z, c])
    pieces = prep(c1, tokens, ids, weights)
    column = lax.all_to_all(pieces, "dp", 0, 0, tiled=True).reshape(ZN * TOK, WIDE)
    packed, shared_own, ext = pack(zc, column)
    shared_oth = lax.ppermute(shared_own, "tensor", SWAP)
    arrived = lax.all_to_all(packed, "expert", 0, 0, tiled=True)
    other = lax.ppermute(arrived, "tensor", SWAP)

    def by_chunk(a):
        a = a.reshape(EXPERTS, ZN, CAP, HALF)
        return jnp.moveaxis(a, 1, 0).reshape(ZN, ROWS, HALF)

    own, oth = by_chunk(arrived), by_chunk(other)
    args = (c1, own, oth, shared_own, shared_oth, wg, wu, sg, su)
    early = up_dots(0, 3, *args)
    late = up_dots(3, 5, *args)
    gate = dict(zip(ORDER, early[:3] + late[:5]))
    up = dict(zip(ORDER, early[3:] + late[5:]))
    g_down = ring([gate[k] for k in (4, 3, 2, 1)], -1)
    u_up = ring([up[k] for k in (4, 5, 6, 7)], 1)
    u_down = ring([up[k] for k in (3, 2, 1)], -1)
    g_up = ring([gate[k] for k in (5, 6, 7)], 1)
    g = (gate[0] + (g_down + g_up)) * (1.0 / SCALE)
    u = (up[0] + (u_down + u_up)) * (1.0 / SCALE)
    hidden = (jax.nn.silu(g) * u).astype(jnp.bfloat16)
    got = {0: hidden}
    down, above = hidden, hidden
    for j in range(1, 4):
        down = lax.ppermute(down, "dp", shifted(-1))
        above = lax.ppermute(above, "dp", shifted(1))
        got[ZN - j], got[j] = down, above
    cut = CHUNK // 2
    down = lax.ppermute(down[:cut], "dp", shifted(-1))
    above = lax.ppermute(above[cut:], "dp", shifted(1))
    got[4] = jnp.concatenate([down, above])
    held = {}
    for a, b, sends in (((7, 6), (1, 2), ((1, 1), (2, 2))), ((5, 0), (3, 4), ((3, 3), (0, 4)))):
        keep, send = down_dots(c1, [got[k] for k in a + b], wd, sd)
        total = keep + lax.ppermute(send, "tensor", SWAP)
        rows = total[:, :ROWS].astype(jnp.bfloat16).reshape(2, EXPERTS, CAP, BLOCK)
        rows = jnp.moveaxis(rows, 0, 1).reshape(EXPERTS, 2 * CAP, BLOCK)
        back = lax.all_to_all(rows, "expert", 0, 0, tiled=True).reshape(2 * ROWS, BLOCK)
        ks = jnp.where(c == 0, jnp.array(a), jnp.array(b))
        shared = total[:, ROWS:].reshape(2 * PADT, BLOCK)
        mixed = combine((z - ks) % ZN, ext, back, shared)
        for i, (to, fro) in enumerate(sends):
            held[to] = lax.ppermute(mixed[i * PADT : (i + 1) * PADT], ("dp", "tensor"), paired(to, fro))
    parts = [held[1], held[2], held[3], held[0]]
    others = []
    for p in parts:
        others.append(lax.ppermute(p, "tensor", SWAP))
    return assemble(zc, *parts, *others)


def solution(mesh):
    placed = (
        P(("dp", "expert"), None),
        P(("dp", "expert"), None),
        P(("dp", "expert"), None),
        P("expert", "dp", "tensor"),
        P("expert", "dp", "tensor"),
        P("expert", "tensor", "dp"),
        P("dp", "tensor"),
        P("dp", "tensor"),
        P("tensor", "dp"),
    )
    return jax.shard_map(
        layer, mesh=mesh, in_specs=placed, out_specs=P(("dp", "expert"), None), check_vma=False
    )
```

```python
import functools

import jax
import jax.numpy as jnp
from jax import lax
from jax.experimental import pallas as pl
from jax.experimental.pallas import tpu as pltpu
from jax.sharding import PartitionSpec as P

EXPERTS = 16
CAP = 8
TOP = 8
ZN = 8
TOK = 12
PADT = 16
BLOCK = 896
HALF = 448
WIDE = 512
ROWS = EXPERTS * CAP
CHUNK = ROWS + PADT
FFH = 1024
EARLY = 3
CUT = FFH // 2
NT = 256
ORDER = (3, 4, 5, 6, 7, 0, 1, 2)
SCALE = 16.0
LINK = jnp.float16

PARAMS = pltpu.CompilerParams(vmem_limit_bytes=16 * 1024 * 1024)
VMEM = pl.BlockSpec(memory_space=pltpu.VMEM)
SMEM = pl.BlockSpec(memory_space=pltpu.SMEM)
SWAP = [(0, 1), (1, 0)]


def shifted(k):
    return [(i, (i + k) % ZN) for i in range(ZN)]


def paired(up, down):
    out = []
    for i in range(ZN):
        out.append((i * 2, ((i + up) % ZN) * 2))
        out.append((i * 2 + 1, ((i - down) % ZN) * 2 + 1))
    return out


def fdot(a, b):
    return jnp.dot(a, b, preferred_element_type=jnp.float32)


def prep_kernel(c_ref, x_hbm, ids_hbm, w_hbm, out_ref, x_ref, ids_ref, w_ref, sems):
    first = c_ref[0] == 0
    pairs = ((ids_hbm, ids_ref), (w_hbm, w_ref), (x_hbm, x_ref))
    copies = [pltpu.make_async_copy(a, b, sems.at[i]) for i, (a, b) in enumerate(pairs)]
    for copy in copies:
        copy.start()
    for copy in copies:
        copy.wait()
    w = w_ref[...]
    hi = w.astype(jnp.bfloat16)
    rest = w - hi.astype(jnp.float32)
    mid = rest.astype(jnp.bfloat16)
    low = (rest - mid.astype(jnp.float32)).astype(jnp.bfloat16)
    lane = lax.broadcasted_iota(jnp.int32, (TOP, 128), 1)
    part = lax.broadcasted_iota(jnp.int32, (TOP, 128), 0)
    start = jnp.where(first, 64, 0)
    ext = jnp.zeros((TOK, 128), jnp.float32)
    for i, v in enumerate((ids_ref[...].astype(jnp.float32).astype(jnp.bfloat16), hi, mid, low)):
        spread = (lane == start + TOP * i + part).astype(jnp.bfloat16)
        ext = ext + lax.dot_general(v, spread, (((0,), (0,)), ((), ())), preferred_element_type=jnp.float32)
    lanes = lax.broadcasted_iota(jnp.int32, (TOK, 128), 1)
    routing = lanes // 64 == jnp.where(first, 1, 0)
    for b in range(ZN):
        at = b * BLOCK

        @pl.when(first)
        def _():
            out_ref[b, :, :384] = x_ref[:, at : at + 384]
            edge = x_ref[:, at + 384 : at + 512].astype(jnp.float32)
            out_ref[b, :, 384:] = jnp.where(routing, ext, edge).astype(jnp.bfloat16)

        @pl.when(jnp.logical_not(first))
        def _():
            edge = x_ref[:, at + 384 : at + 512].astype(jnp.float32)
            out_ref[b, :, :128] = jnp.where(routing, ext, edge).astype(jnp.bfloat16)
            out_ref[b, :, 128:] = x_ref[:, at + 512 : at + BLOCK]


def prep(c, x, ids, w):
    return pl.pallas_call(
        prep_kernel,
        out_shape=jax.ShapeDtypeStruct((ZN, TOK, WIDE), jnp.bfloat16),
        in_specs=[SMEM] + [pl.BlockSpec(memory_space=pltpu.HBM)] * 3,
        out_specs=VMEM,
        scratch_shapes=[
            pltpu.VMEM((TOK, ZN * BLOCK), jnp.bfloat16),
            pltpu.VMEM((TOP, TOK), jnp.int32),
            pltpu.VMEM((TOP, TOK), jnp.float32),
            pltpu.SemaphoreType.DMA((3,)),
        ],
        compiler_params=PARAMS,
        name="prep",
    )(c, x, ids, w)


def pack_kernel(s_ref, x_ref, packed_ref, shared_ref, ext_ref):
    z = s_ref[0]
    n = ZN * TOK
    x = x_ref[...].astype(jnp.float32)
    x = jnp.where(s_ref[1] == 0, x, pltpu.roll(x, WIDE - 64, 1))
    ext = x[:, WIDE - 128 :]
    ext_ref[...] = ext.astype(jnp.bfloat16)
    x = x.astype(jnp.bfloat16)[:, :HALF]
    ids = jnp.transpose(ext)[64:72, :].astype(jnp.int32)
    experts = lax.broadcasted_iota(jnp.int32, (EXPERTS, n), 0)
    member = jnp.zeros((EXPERTS, n), jnp.float32)
    for k in range(TOP):
        member = member + (experts == ids[k : k + 1, :]).astype(jnp.float32)
    r0 = lax.broadcasted_iota(jnp.int32, (n, n), 0)
    r1 = lax.broadcasted_iota(jnp.int32, (n, n), 1)
    before = ((r0 // TOK == r1 // TOK) & (r0 < r1)).astype(jnp.bfloat16)
    pos = fdot(member.astype(jnp.bfloat16), before).astype(jnp.int32)
    row = lax.broadcasted_iota(jnp.int32, (1, n), 1)
    zs = row // TOK
    place = (z - zs + 13) % ZN
    target = jnp.where(member > 0.5, place * CAP + pos, -1)
    wanted = lax.broadcasted_iota(jnp.int32, (ZN * CAP, n), 0)
    for e in range(EXPERTS):
        pick = (wanted == target[e : e + 1, :]).astype(jnp.bfloat16)
        packed_ref[e] = fdot(pick, x).astype(jnp.bfloat16)
    wide = lax.broadcasted_iota(jnp.int32, (ZN * PADT, n), 0)
    pick = (wide == place * PADT + row - zs * TOK).astype(jnp.bfloat16)
    shared_ref[...] = fdot(pick, x).astype(jnp.bfloat16)


def pack(s, x):
    return pl.pallas_call(
        pack_kernel,
        out_shape=(
            jax.ShapeDtypeStruct((EXPERTS, ZN * CAP, HALF), jnp.bfloat16),
            jax.ShapeDtypeStruct((ZN * PADT, HALF), jnp.bfloat16),
            jax.ShapeDtypeStruct((ZN * TOK, 128), jnp.bfloat16),
        ),
        in_specs=[SMEM, VMEM],
        out_specs=(VMEM, VMEM, VMEM),
        compiler_params=PARAMS,
        name="pack",
    )(s, x)


def up_kernel(first, count, c_ref, own_ref, oth_ref, so_ref, st_ref, wg_ref, wu_ref, sg_ref, su_ref, *out_refs):
    c = c_ref[0]
    mine = pl.ds(pl.multiple_of(c * HALF, 64), HALF)
    other = pl.ds(pl.multiple_of((1 - c) * HALF, 64), HALF)
    own = own_ref[first : first + count].reshape(count * ROWS, HALF)
    oth = oth_ref[first : first + count].reshape(count * ROWS, HALF)
    so = so_ref[first * PADT : (first + count) * PADT]
    st = st_ref[first * PADT : (first + count) * PADT]
    for w_ref, s_ref, o_refs in ((wg_ref, sg_ref, out_refs[:count]), (wu_ref, su_ref, out_refs[count:])):
        full = (fdot(own, w_ref[0, mine, :]) + fdot(oth, w_ref[0, other, :])) * SCALE
        shared = (fdot(so, s_ref[mine, :]) + fdot(st, s_ref[other, :])) * SCALE
        for i in range(count):
            o_refs[i][:ROWS, :] = full[i * ROWS : (i + 1) * ROWS]
            o_refs[i][ROWS:, :] = shared[i * PADT : (i + 1) * PADT]


def up_dots(first, count, c, own, oth, so, st, wg, wu, sg, su):
    whole = lambda *shape: pl.BlockSpec(shape, lambda n: (0,) * len(shape))
    return pl.pallas_call(
        functools.partial(up_kernel, first, count),
        grid=(FFH // NT,),
        out_shape=(jax.ShapeDtypeStruct((CHUNK, FFH), jnp.float32),) * (2 * count),
        in_specs=[
            SMEM,
            whole(ZN, ROWS, HALF),
            whole(ZN, ROWS, HALF),
            whole(ZN * PADT, HALF),
            whole(ZN * PADT, HALF),
            pl.BlockSpec((1, BLOCK, NT), lambda n: (0, 0, n)),
            pl.BlockSpec((1, BLOCK, NT), lambda n: (0, 0, n)),
            pl.BlockSpec((BLOCK, NT), lambda n: (0, n)),
            pl.BlockSpec((BLOCK, NT), lambda n: (0, n)),
        ],
        out_specs=(pl.BlockSpec((CHUNK, NT), lambda n: (0, n)),) * (2 * count),
        compiler_params=PARAMS,
        cost_estimate=pl.CostEstimate(
            flops=2 * 2 * count * CHUNK * BLOCK * FFH, bytes_accessed=4 * BLOCK * FFH * 2, transcendentals=0
        ),
    )(c, own, oth, so, st, wg, wu, sg, su)


def down_kernel(c_ref, *refs):
    xs, (wd_ref, sd_ref, keep_ref, send_ref) = refs[:-4], refs[-4:]
    sides = (xs[::2], xs[1::2])
    n = len(xs) // 4
    full, shared = 0.0, 0.0
    for side, cols in zip(sides, (slice(0, CUT), slice(CUT, FFH))):
        full = full + fdot(jnp.concatenate([x[:ROWS] for x in side], axis=0), wd_ref[0, cols])
        shared = shared + fdot(jnp.concatenate([x[ROWS:] for x in side], axis=0), sd_ref[cols])

    def store(ref, i, at):
        ref[i, :ROWS] = full[at * ROWS : (at + 1) * ROWS]
        ref[i, ROWS:] = shared[at * PADT : (at + 1) * PADT]

    @pl.when(c_ref[0] == 0)
    def _():
        for i in range(n):
            store(keep_ref, i, i)
            store(send_ref, i, n + i)

    @pl.when(c_ref[0] != 0)
    def _():
        for i in range(n):
            store(keep_ref, i, n + i)
            store(send_ref, i, i)


def down_dots(c, xs, wd, sd):
    n = len(xs) // 4
    return pl.pallas_call(
        down_kernel,
        out_shape=(
            jax.ShapeDtypeStruct((n, CHUNK, BLOCK), jnp.float32),
            jax.ShapeDtypeStruct((n, CHUNK, BLOCK), jnp.float32),
        ),
        in_specs=[SMEM] + [VMEM] * (len(xs) + 2),
        out_specs=(VMEM, VMEM),
        compiler_params=PARAMS,
        cost_estimate=pl.CostEstimate(
            flops=2 * 2 * n * CHUNK * BLOCK * FFH, bytes_accessed=2 * BLOCK * FFH * 2, transcendentals=0
        ),
        name="down_dots",
    )(c, *xs, wd, sd)


def settle_kernel(keep_ref, came_ref, *refs):
    before, (rows_ref, shared_ref) = refs[:-2], refs[-2:]
    at = 0
    if before:
        at = 2 * CAP
        rows_ref[:, :at, :] = before[0][...]
    for i in range(2):
        total = keep_ref[i, :ROWS] + came_ref[i, :ROWS]
        rows_ref[:, at + i * CAP : at + (i + 1) * CAP, :] = total.reshape(EXPERTS, CAP, BLOCK).astype(jnp.bfloat16)
        shared_ref[i * PADT : (i + 1) * PADT] = keep_ref[i, ROWS:] + came_ref[i, ROWS:]


def settle(keep, came, *before):
    return pl.pallas_call(
        settle_kernel,
        out_shape=(
            jax.ShapeDtypeStruct((EXPERTS, (2 + 2 * len(before)) * CAP, BLOCK), jnp.bfloat16),
            jax.ShapeDtypeStruct((2 * PADT, BLOCK), jnp.float32),
        ),
        in_specs=[VMEM] * (2 + len(before)),
        out_specs=(VMEM, VMEM),
        compiler_params=PARAMS,
        name="settle",
    )(keep, came, *before)


def combine_kernel(zs_ref, ext_ref, back_ref, near_ref, far_ref, out_ref):
    n = ZN * TOK
    rows = 4 * PADT
    cols = 4 * ROWS
    t = lax.broadcasted_iota(jnp.int32, (rows, n), 0)
    r = lax.broadcasted_iota(jnp.int32, (rows, n), 1)
    zs = jnp.full((rows, n), zs_ref[3], jnp.int32)
    for i in range(3):
        zs = jnp.where(t // PADT == i, zs_ref[i], zs)
    pick = ((r == zs * TOK + t % PADT) & (t % PADT < TOK)).astype(jnp.bfloat16)
    ext = fdot(pick, ext_ref[...])
    weight = (ext[:, 72:80] + ext[:, 80:88]) + ext[:, 88:96]
    column = lax.broadcasted_iota(jnp.int32, (rows, cols), 1)
    row = lax.broadcasted_iota(jnp.int32, (rows, cols), 0)
    live = (row % PADT < TOK) & (row // PADT == (column // CAP) % 4)
    owner = (column // (4 * CAP)).astype(jnp.float32)
    slot = (column % CAP).astype(jnp.float32)
    member = jnp.zeros((rows, cols), jnp.float32)
    scale = jnp.zeros((rows, cols), jnp.float32)
    for k in range(TOP):
        hit = (ext[:, 64 + k : 65 + k] == owner) & live
        member = jnp.where(hit, 1.0, member)
        scale = jnp.where(hit, weight[:, k : k + 1], scale)
    i0 = lax.broadcasted_iota(jnp.int32, (rows, rows), 0)
    i1 = lax.broadcasted_iota(jnp.int32, (rows, rows), 1)
    before = ((i1 < i0) & (i0 // PADT == i1 // PADT)).astype(jnp.bfloat16)
    pos = fdot(before, member.astype(jnp.bfloat16))
    scale = jnp.where((pos == slot) & (member > 0.5), scale, 0.0)
    hi = scale.astype(jnp.bfloat16)
    rest = scale - hi.astype(jnp.float32)
    mid = rest.astype(jnp.bfloat16)
    low = (rest - mid.astype(jnp.float32)).astype(jnp.bfloat16)
    back = back_ref[...]
    total = (fdot(low, back) + fdot(mid, back)) + fdot(hi, back)
    out_ref[: 2 * PADT] = (near_ref[...] + total[: 2 * PADT]).astype(jnp.bfloat16)
    out_ref[2 * PADT :] = (far_ref[...] + total[2 * PADT :]).astype(jnp.bfloat16)


def combine(zs, ext, back, near, far):
    return pl.pallas_call(
        combine_kernel,
        out_shape=jax.ShapeDtypeStruct((4 * PADT, BLOCK), jnp.bfloat16),
        in_specs=[SMEM, VMEM, VMEM, VMEM, VMEM],
        out_specs=VMEM,
        compiler_params=PARAMS,
        name="combine",
    )(zs, ext, back, near, far)


def assemble_kernel(s_ref, *refs):
    out_ref = refs[-1]
    z = s_ref[0]
    held_ref, came_ref = refs[:-1]
    a1, a2, b3, b0 = [held_ref[i * PADT : i * PADT + TOK] for i in range(4)]
    o1, o2, o3, o0 = [came_ref[i * PADT : i * PADT + TOK] for i in range(4)]

    def put(parts):
        for i, part in enumerate(parts):
            at = pl.multiple_of(((z + i) % ZN) * BLOCK, 128)
            out_ref[:, pl.ds(at, BLOCK)] = part

    @pl.when(s_ref[1] == 0)
    def _():
        put((b0, o1, o2, o3, o0, b3, a2, a1))

    @pl.when(s_ref[1] != 0)
    def _():
        put((o0, a1, a2, b3, b0, o3, o2, o1))


def assemble(s, *parts):
    return pl.pallas_call(
        assemble_kernel,
        out_shape=jax.ShapeDtypeStruct((TOK, ZN * BLOCK), jnp.bfloat16),
        in_specs=[SMEM] + [VMEM] * len(parts),
        out_specs=VMEM,
        compiler_params=PARAMS,
        name="assemble",
    )(s, *parts)


def ring(parts, shift):
    total = None
    for mine in parts:
        total = mine if total is None else mine + total.astype(jnp.float32)
        total = lax.ppermute(total.astype(LINK), "dp", shifted(shift))
    return total.astype(jnp.float32)


def layer(tokens, ids, weights, wg, wu, wd, sg, su, sd):
    z = lax.axis_index("dp")
    c = lax.axis_index("tensor")
    c1, zc = c.reshape(1), jnp.stack([z, c])
    pieces = prep(c1, tokens, ids.T, weights.T)
    column = lax.all_to_all(pieces, "dp", 0, 0, tiled=True).reshape(ZN * TOK, WIDE)
    packed, shared_own, ext = pack(zc, column)
    shared_oth = lax.ppermute(shared_own, "tensor", SWAP)
    arrived = lax.all_to_all(packed, "expert", 0, 0, tiled=True)
    other = lax.ppermute(arrived, "tensor", SWAP)
    own, oth = [
        jnp.moveaxis(a.reshape(EXPERTS, ZN, CAP, HALF), 1, 0).reshape(ZN, ROWS, HALF) for a in (arrived, other)
    ]
    args = (c1, own, oth, shared_own, shared_oth, wg, wu, sg, su)
    early = up_dots(0, EARLY, *args)
    late = up_dots(EARLY, ZN - EARLY, *args)
    gate = dict(zip(ORDER, early[:EARLY] + late[: ZN - EARLY]))
    up = dict(zip(ORDER, early[EARLY:] + late[ZN - EARLY :]))
    g_down = ring([gate[k] for k in (4, 3, 2, 1)], -1)
    u_up = ring([up[k] for k in (4, 5, 6, 7)], 1)
    u_down = ring([up[k] for k in (3, 2, 1)], -1)
    g_up = ring([gate[k] for k in (5, 6, 7)], 1)
    g = (gate[0] + (g_down + g_up)) * (1.0 / SCALE)
    u = (up[0] + (u_down + u_up)) * (1.0 / SCALE)
    hidden = (jax.nn.silu(g) * u).astype(jnp.bfloat16)
    top, tail = hidden[:, :CUT], hidden[:, CUT:]
    got = {0: (top, tail)}
    pd, pu, qd, qu = top, top, tail, tail
    for j in range(1, 5):
        pd = lax.ppermute(pd, "dp", shifted(-1))
        qu = lax.ppermute(qu, "dp", shifted(1))
        if j < 4:
            qd = lax.ppermute(qd, "dp", shifted(-1))
            pu = lax.ppermute(pu, "dp", shifted(1))
            got[ZN - j], got[j] = (pd, qd), (pu, qu)
        else:
            got[4] = (pd, qu)
    rows, shares = (), []
    for a, b in (((7, 6), (1, 2)), ((5, 0), (3, 4))):
        keep, send = down_dots(c1, [p for k in a + b for p in got[k]], wd, sd)
        came = lax.ppermute(send, "tensor", SWAP)
        *rows, shared = settle(keep, came, *rows)
        shares.append(shared)
    back = lax.all_to_all(rows[0], "expert", 0, 0, tiled=True).reshape(4 * ROWS, BLOCK)
    ks = jnp.where(c == 0, jnp.array((7, 6, 5, 0)), jnp.array((1, 2, 3, 4)))
    mixed = combine((z - ks) % ZN, ext, back, *shares)
    held = []
    for i, (to, fro) in enumerate(((1, 1), (2, 2), (3, 3), (0, 4))):
        held.append(lax.ppermute(mixed[i * PADT : (i + 1) * PADT], ("dp", "tensor"), paired(to, fro)))
    held = jnp.concatenate(held)
    others = lax.ppermute(held, "tensor", SWAP)
    return assemble(zc, held, others)


def solution(mesh):
    placed = (
        P(("dp", "expert"), None),
        P(("dp", "expert"), None),
        P(("dp", "expert"), None),
        P("expert", "dp", "tensor"),
        P("expert", "dp", "tensor"),
        P("expert", "tensor", "dp"),
        P("dp", "tensor"),
        P("dp", "tensor"),
        P("tensor", "dp"),
    )
    return jax.shard_map(layer, mesh=mesh, in_specs=placed, out_specs=P(("dp", "expert"), None), check_vma=False)
```

```python
import functools

import jax
import jax.numpy as jnp
from jax import lax
from jax.experimental import pallas as pl
from jax.experimental.pallas import tpu as pltpu
from jax.sharding import PartitionSpec as P

EXPERTS = 16
CAP = 8
TOP = 8
ZN = 8
TOK = 12
PADT = 16
BLOCK = 896
ROWS = EXPERTS * CAP
CHUNK = ROWS + PADT
FFH = 1024
CUT = FFH // 2
NT = 256
EXT = 128
HELD = ((0, 7, 6, 5), (4, 1, 2, 3))
EARLY = (3, 4, 5)
LATE = (6, 7, 0, 1, 2)
SCALE = 16.0
LINK = jnp.float16

PARAMS = pltpu.CompilerParams(vmem_limit_bytes=16 * 1024 * 1024)
VMEM = pl.BlockSpec(memory_space=pltpu.VMEM)
SMEM = pl.BlockSpec(memory_space=pltpu.SMEM)
SWAP = [(0, 1), (1, 0)]


def shifted(k):
    return [(i, (i + k) % ZN) for i in range(ZN)]


def paired(up, down):
    out = []
    for i in range(ZN):
        out.append((i * 2, ((i + up) % ZN) * 2))
        out.append((i * 2 + 1, ((i - down) % ZN) * 2 + 1))
    return out


def fdot(a, b):
    return jnp.dot(a, b, preferred_element_type=jnp.float32)


def prep_kernel(s_ref, x_hbm, ids_hbm, w_hbm, *refs):
    outs, (x_ref, ids_ref, w_ref, sems) = refs[:4], refs[4:]
    z, c = s_ref[0], s_ref[1]
    pairs = ((ids_hbm, ids_ref), (w_hbm, w_ref), (x_hbm, x_ref))
    copies = [pltpu.make_async_copy(a, b, sems.at[i]) for i, (a, b) in enumerate(pairs)]
    for copy in copies:
        copy.start()
    for copy in copies:
        copy.wait()
    w = w_ref[...]
    hi = w.astype(jnp.bfloat16)
    rest = w - hi.astype(jnp.float32)
    mid = rest.astype(jnp.bfloat16)
    low = (rest - mid.astype(jnp.float32)).astype(jnp.bfloat16)
    lane = lax.broadcasted_iota(jnp.int32, (TOP, EXT), 1)
    part = lax.broadcasted_iota(jnp.int32, (TOP, EXT), 0)
    ext = jnp.zeros((TOK, EXT), jnp.float32)
    for i, v in enumerate((ids_ref[...].astype(jnp.float32).astype(jnp.bfloat16), hi, mid, low)):
        spread = (lane == TOP * i + part).astype(jnp.bfloat16)
        ext = ext + lax.dot_general(v, spread, (((0,), (0,)), ((), ())), preferred_element_type=jnp.float32)
    ext = ext.astype(jnp.bfloat16)
    for j, out_ref in enumerate(outs):
        block = (z + 4 * c) % ZN if j == 0 else (z + ZN + jnp.where(c == 0, -j, j)) % ZN
        out_ref[...] = jnp.zeros((PADT, BLOCK + EXT), jnp.bfloat16)
        out_ref[:TOK, :BLOCK] = x_ref[:, pl.ds(pl.multiple_of(block * BLOCK, 128), BLOCK)]
        out_ref[:TOK, BLOCK:] = ext


def prep(s, x, ids, w):
    return pl.pallas_call(
        prep_kernel,
        out_shape=(jax.ShapeDtypeStruct((PADT, BLOCK + EXT), jnp.bfloat16),) * 4,
        in_specs=[SMEM] + [pl.BlockSpec(memory_space=pltpu.HBM)] * 3,
        out_specs=(VMEM,) * 4,
        scratch_shapes=[
            pltpu.VMEM((TOK, ZN * BLOCK), jnp.bfloat16),
            pltpu.VMEM((TOP, TOK), jnp.int32),
            pltpu.VMEM((TOP, TOK), jnp.float32),
            pltpu.SemaphoreType.DMA((3,)),
        ],
        compiler_params=PARAMS,
        name="prep",
    )(s, x, ids, w)


def pack_kernel(*refs):
    xs, (packed_ref, shared_ref, ext_ref) = refs[:4], refs[4:]
    n = 4 * PADT
    for i, x in enumerate(xs):
        shared_ref[i * PADT : (i + 1) * PADT] = x[:, :BLOCK]
        ext_ref[i * PADT : (i + 1) * PADT] = x[:, BLOCK:]
    x = shared_ref[...]
    ids = jnp.transpose(ext_ref[...].astype(jnp.float32))[:TOP, :].astype(jnp.int32)
    experts = lax.broadcasted_iota(jnp.int32, (EXPERTS, n), 0)
    row = lax.broadcasted_iota(jnp.int32, (EXPERTS, n), 1)
    member = jnp.zeros((EXPERTS, n), jnp.float32)
    for k in range(TOP):
        member = member + ((experts == ids[k : k + 1, :]) & (row % PADT < TOK)).astype(jnp.float32)
    r0 = lax.broadcasted_iota(jnp.int32, (n, n), 0)
    r1 = lax.broadcasted_iota(jnp.int32, (n, n), 1)
    before = ((r0 // PADT == r1 // PADT) & (r0 < r1)).astype(jnp.bfloat16)
    pos = fdot(member.astype(jnp.bfloat16), before).astype(jnp.int32)
    target = jnp.where(member > 0.5, row // PADT * CAP + pos, -1)
    wanted = lax.broadcasted_iota(jnp.int32, (4 * CAP, n), 0)
    for e in range(EXPERTS):
        pick = (wanted == target[e : e + 1, :]).astype(jnp.bfloat16)
        packed_ref[e] = fdot(pick, x).astype(jnp.bfloat16)


def pack(*xs):
    return pl.pallas_call(
        pack_kernel,
        out_shape=(
            jax.ShapeDtypeStruct((EXPERTS, 4 * CAP, BLOCK), jnp.bfloat16),
            jax.ShapeDtypeStruct((4 * PADT, BLOCK), jnp.bfloat16),
            jax.ShapeDtypeStruct((4 * PADT, EXT), jnp.bfloat16),
        ),
        in_specs=[VMEM] * 4,
        out_specs=(VMEM, VMEM, VMEM),
        compiler_params=PARAMS,
        name="pack",
    )(*xs)


def up_kernel(ks, c_ref, own_ref, oth_ref, so_ref, st_ref, wg_ref, wu_ref, sg_ref, su_ref, *refs):
    count = len(ks)
    out_refs, (x_ref, s_ref) = refs[:-2], refs[-2:]

    def gather(sides):
        for at, k in enumerate(ks):
            side = 0 if k in HELD[0] else 1
            i = HELD[side].index(k)
            full, shared = sides[side]
            x_ref[at * ROWS : (at + 1) * ROWS] = full[i]
            s_ref[at * PADT : (at + 1) * PADT] = shared[i * PADT : (i + 1) * PADT]

    own, oth = (own_ref, so_ref), (oth_ref, st_ref)
    start = pl.program_id(0) == 0

    @pl.when(start & (c_ref[0] == 0))
    def _():
        gather((own, oth))

    @pl.when(start & (c_ref[0] != 0))
    def _():
        gather((oth, own))

    for w_ref, v_ref, o_refs in ((wg_ref, sg_ref, out_refs[:count]), (wu_ref, su_ref, out_refs[count:])):
        full = fdot(x_ref[...], w_ref[0]) * SCALE
        shared = fdot(s_ref[...], v_ref[...]) * SCALE
        for i in range(count):
            o_refs[i][:ROWS, :] = full[i * ROWS : (i + 1) * ROWS]
            o_refs[i][ROWS:, :] = shared[i * PADT : (i + 1) * PADT]


def up_dots(ks, c, own, oth, so, st, wg, wu, sg, su):
    whole = lambda *shape: pl.BlockSpec(shape, lambda n: (0,) * len(shape))
    count = len(ks)
    return pl.pallas_call(
        functools.partial(up_kernel, ks),
        grid=(FFH // NT,),
        out_shape=(jax.ShapeDtypeStruct((CHUNK, FFH), jnp.float32),) * (2 * count),
        in_specs=[
            SMEM,
            whole(4, ROWS, BLOCK),
            whole(4, ROWS, BLOCK),
            whole(4 * PADT, BLOCK),
            whole(4 * PADT, BLOCK),
            pl.BlockSpec((1, BLOCK, NT), lambda n: (0, 0, n)),
            pl.BlockSpec((1, BLOCK, NT), lambda n: (0, 0, n)),
            pl.BlockSpec((BLOCK, NT), lambda n: (0, n)),
            pl.BlockSpec((BLOCK, NT), lambda n: (0, n)),
        ],
        out_specs=(pl.BlockSpec((CHUNK, NT), lambda n: (0, n)),) * (2 * count),
        scratch_shapes=[
            pltpu.VMEM((count * ROWS, BLOCK), jnp.bfloat16),
            pltpu.VMEM((count * PADT, BLOCK), jnp.bfloat16),
        ],
        compiler_params=PARAMS,
        cost_estimate=pl.CostEstimate(
            flops=2 * 2 * count * CHUNK * BLOCK * FFH, bytes_accessed=4 * BLOCK * FFH * 2, transcendentals=0
        ),
    )(c, own, oth, so, st, wg, wu, sg, su)


def down_kernel(c_ref, *refs):
    xs, (wd_ref, sd_ref, keep_ref, send_ref) = refs[:-4], refs[-4:]
    sides = (xs[::2], xs[1::2])
    n = len(xs) // 4
    full, shared = 0.0, 0.0
    for side, cols in zip(sides, (slice(0, CUT), slice(CUT, FFH))):
        full = full + fdot(jnp.concatenate([x[:ROWS] for x in side], axis=0), wd_ref[0, cols])
        shared = shared + fdot(jnp.concatenate([x[ROWS:] for x in side], axis=0), sd_ref[cols])

    def store(ref, i, at):
        ref[i, :ROWS] = full[at * ROWS : (at + 1) * ROWS]
        ref[i, ROWS:] = shared[at * PADT : (at + 1) * PADT]

    @pl.when(c_ref[0] == 0)
    def _():
        for i in range(n):
            store(keep_ref, i, i)
            store(send_ref, i, n + i)

    @pl.when(c_ref[0] != 0)
    def _():
        for i in range(n):
            store(keep_ref, i, n + i)
            store(send_ref, i, i)


def down_dots(c, xs, wd, sd):
    n = len(xs) // 4
    return pl.pallas_call(
        down_kernel,
        out_shape=(
            jax.ShapeDtypeStruct((n, CHUNK, BLOCK), jnp.float32),
            jax.ShapeDtypeStruct((n, CHUNK, BLOCK), jnp.float32),
        ),
        in_specs=[SMEM] + [VMEM] * (len(xs) + 2),
        out_specs=(VMEM, VMEM),
        compiler_params=PARAMS,
        cost_estimate=pl.CostEstimate(
            flops=2 * 2 * n * CHUNK * BLOCK * FFH, bytes_accessed=2 * BLOCK * FFH * 2, transcendentals=0
        ),
        name="down_dots",
    )(c, *xs, wd, sd)


def settle_kernel(keep_ref, came_ref, *refs):
    before, (rows_ref, shared_ref) = refs[:-2], refs[-2:]
    at = 0
    if before:
        at = 2 * CAP
        rows_ref[:, :at, :] = before[0][...]
    for i in range(2):
        total = keep_ref[i, :ROWS] + came_ref[i, :ROWS]
        rows_ref[:, at + i * CAP : at + (i + 1) * CAP, :] = total.reshape(EXPERTS, CAP, BLOCK).astype(jnp.bfloat16)
        shared_ref[i * PADT : (i + 1) * PADT] = keep_ref[i, ROWS:] + came_ref[i, ROWS:]


def settle(keep, came, *before):
    return pl.pallas_call(
        settle_kernel,
        out_shape=(
            jax.ShapeDtypeStruct((EXPERTS, (2 + 2 * len(before)) * CAP, BLOCK), jnp.bfloat16),
            jax.ShapeDtypeStruct((2 * PADT, BLOCK), jnp.float32),
        ),
        in_specs=[VMEM] * (2 + len(before)),
        out_specs=(VMEM, VMEM),
        compiler_params=PARAMS,
        name="settle",
    )(keep, came, *before)


def combine_kernel(ext_ref, back_ref, near_ref, far_ref, out_ref):
    rows = 4 * PADT
    cols = 4 * ROWS
    ext = jnp.concatenate([ext_ref[PADT:], ext_ref[:PADT]], axis=0).astype(jnp.float32)
    weight = (ext[:, TOP : 2 * TOP] + ext[:, 2 * TOP : 3 * TOP]) + ext[:, 3 * TOP : 4 * TOP]
    column = lax.broadcasted_iota(jnp.int32, (rows, cols), 1)
    row = lax.broadcasted_iota(jnp.int32, (rows, cols), 0)
    live = (row % PADT < TOK) & (row // PADT == (column // CAP) % 4)
    owner = (column // (4 * CAP)).astype(jnp.float32)
    slot = (column % CAP).astype(jnp.float32)
    member = jnp.zeros((rows, cols), jnp.float32)
    scale = jnp.zeros((rows, cols), jnp.float32)
    for k in range(TOP):
        hit = (ext[:, k : k + 1] == owner) & live
        member = jnp.where(hit, 1.0, member)
        scale = jnp.where(hit, weight[:, k : k + 1], scale)
    i0 = lax.broadcasted_iota(jnp.int32, (rows, rows), 0)
    i1 = lax.broadcasted_iota(jnp.int32, (rows, rows), 1)
    before = ((i1 < i0) & (i0 // PADT == i1 // PADT)).astype(jnp.bfloat16)
    pos = fdot(before, member.astype(jnp.bfloat16))
    scale = jnp.where((pos == slot) & (member > 0.5), scale, 0.0)
    hi = scale.astype(jnp.bfloat16)
    rest = scale - hi.astype(jnp.float32)
    mid = rest.astype(jnp.bfloat16)
    low = (rest - mid.astype(jnp.float32)).astype(jnp.bfloat16)
    back = back_ref[...]
    total = (fdot(low, back) + fdot(mid, back)) + fdot(hi, back)
    out_ref[: 2 * PADT] = (near_ref[...] + total[: 2 * PADT]).astype(jnp.bfloat16)
    out_ref[2 * PADT :] = (far_ref[...] + total[2 * PADT :]).astype(jnp.bfloat16)


def combine(ext, back, near, far):
    return pl.pallas_call(
        combine_kernel,
        out_shape=jax.ShapeDtypeStruct((4 * PADT, BLOCK), jnp.bfloat16),
        in_specs=[VMEM, VMEM, VMEM, VMEM],
        out_specs=VMEM,
        compiler_params=PARAMS,
        name="combine",
    )(ext, back, near, far)


def assemble_kernel(s_ref, *refs):
    out_ref = refs[-1]
    z = s_ref[0]
    held_ref, came_ref = refs[:-1]
    a1, a2, b3, b0 = [held_ref[i * PADT : i * PADT + TOK] for i in range(4)]
    o1, o2, o3, o0 = [came_ref[i * PADT : i * PADT + TOK] for i in range(4)]

    def put(parts):
        for i, part in enumerate(parts):
            at = pl.multiple_of(((z + i) % ZN) * BLOCK, 128)
            out_ref[:, pl.ds(at, BLOCK)] = part

    @pl.when(s_ref[1] == 0)
    def _():
        put((b0, o1, o2, o3, o0, b3, a2, a1))

    @pl.when(s_ref[1] != 0)
    def _():
        put((o0, a1, a2, b3, b0, o3, o2, o1))


def assemble(s, *parts):
    return pl.pallas_call(
        assemble_kernel,
        out_shape=jax.ShapeDtypeStruct((TOK, ZN * BLOCK), jnp.bfloat16),
        in_specs=[SMEM] + [VMEM] * len(parts),
        out_specs=VMEM,
        compiler_params=PARAMS,
        name="assemble",
    )(s, *parts)


def ring(parts, shift):
    total = None
    for mine in parts:
        total = mine if total is None else mine + total.astype(jnp.float32)
        total = lax.ppermute(total.astype(LINK), "dp", shifted(shift))
    return total.astype(jnp.float32)


def layer(tokens, ids, weights, wg, wu, wd, sg, su, sd):
    z = lax.axis_index("dp")
    c = lax.axis_index("tensor")
    c1, zc = c.reshape(1), jnp.stack([z, c])
    sent = prep(zc, tokens, ids.T, weights.T)
    came = []
    for j, piece in enumerate(sent):
        came.append(lax.ppermute(piece, ("dp", "tensor"), paired(-j, -j) if j else paired(0, 4)))
    packed, shared_own, ext = pack(*came)
    shared_oth = lax.ppermute(shared_own, "tensor", SWAP)
    arrived = lax.all_to_all(packed, "expert", 0, 0, tiled=True)
    other = lax.ppermute(arrived, "tensor", SWAP)
    own, oth = [
        jnp.moveaxis(a.reshape(EXPERTS, 4, CAP, BLOCK), 1, 0).reshape(4, ROWS, BLOCK) for a in (arrived, other)
    ]
    args = (c1, own, oth, shared_own, shared_oth, wg, wu, sg, su)
    early = up_dots(EARLY, *args)
    late = up_dots(LATE, *args)
    gate = dict(zip(EARLY + LATE, early[: len(EARLY)] + late[: len(LATE)]))
    up = dict(zip(EARLY + LATE, early[len(EARLY) :] + late[len(LATE) :]))
    g_down = ring([gate[k] for k in (4, 3, 2, 1)], -1)
    u_up = ring([up[k] for k in (4, 5, 6, 7)], 1)
    u_down = ring([up[k] for k in (3, 2, 1)], -1)
    g_up = ring([gate[k] for k in (5, 6, 7)], 1)
    g = (gate[0] + (g_down + g_up)) * (1.0 / SCALE)
    u = (up[0] + (u_down + u_up)) * (1.0 / SCALE)
    hidden = (jax.nn.silu(g) * u).astype(jnp.bfloat16)
    top, tail = hidden[:, :CUT], hidden[:, CUT:]
    got = {0: (top, tail)}
    pd, pu, qd, qu = top, top, tail, tail
    for j in range(1, 5):
        pd = lax.ppermute(pd, "dp", shifted(-1))
        qu = lax.ppermute(qu, "dp", shifted(1))
        if j < 4:
            qd = lax.ppermute(qd, "dp", shifted(-1))
            pu = lax.ppermute(pu, "dp", shifted(1))
            got[ZN - j], got[j] = (pd, qd), (pu, qu)
        else:
            got[4] = (pd, qu)
    rows, shares = (), []
    for a, b in (((7, 6), (1, 2)), ((5, 0), (3, 4))):
        keep, send = down_dots(c1, [p for k in a + b for p in got[k]], wd, sd)
        came = lax.ppermute(send, "tensor", SWAP)
        *rows, shared = settle(keep, came, *rows)
        shares.append(shared)
    back = lax.all_to_all(rows[0], "expert", 0, 0, tiled=True).reshape(4 * ROWS, BLOCK)
    mixed = combine(ext, back, *shares)
    held = []
    for i, (to, fro) in enumerate(((1, 1), (2, 2), (3, 3), (0, 4))):
        held.append(lax.ppermute(mixed[i * PADT : (i + 1) * PADT], ("dp", "tensor"), paired(to, fro)))
    held = jnp.concatenate(held)
    others = lax.ppermute(held, "tensor", SWAP)
    return assemble(zc, held, others)


def solution(mesh):
    placed = (
        P(("dp", "expert"), None),
        P(("dp", "expert"), None),
        P(("dp", "expert"), None),
        P("expert", "dp", "tensor"),
        P("expert", "dp", "tensor"),
        P("expert", "tensor", "dp"),
        P("dp", "tensor"),
        P("dp", "tensor"),
        P("tensor", "dp"),
    )
    return jax.shard_map(layer, mesh=mesh, in_specs=placed, out_specs=P(("dp", "expert"), None), check_vma=False)
```

```python
import functools

import jax
import jax.numpy as jnp
from jax import lax
from jax.experimental import pallas as pl
from jax.experimental.pallas import tpu as pltpu
from jax.sharding import PartitionSpec as P

EXPERTS = 16
CAP = 8
TOP = 8
ZN = 8
TOK = 12
PADT = 16
BLOCK = 896
ROWS = EXPERTS * CAP
CHUNK = ROWS + PADT
FFH = 1024
CUT = FFH // 2
NT = 256
EXT = 128
HELD = ((0, 7, 6, 5), (4, 1, 2, 3))
EARLY = (3, 4, 5)
LATE = (6, 7, 0, 1, 2)
SCALE = 16.0
LINK = jnp.float16

PARAMS = pltpu.CompilerParams(vmem_limit_bytes=16 * 1024 * 1024)
VMEM = pl.BlockSpec(memory_space=pltpu.VMEM)
SMEM = pl.BlockSpec(memory_space=pltpu.SMEM)
SWAP = [(0, 1), (1, 0)]


def shifted(k):
    return [(i, (i + k) % ZN) for i in range(ZN)]


def paired(up, down):
    out = []
    for i in range(ZN):
        out.append((i * 2, ((i + up) % ZN) * 2))
        out.append((i * 2 + 1, ((i - down) % ZN) * 2 + 1))
    return out


def fdot(a, b):
    return jnp.dot(a, b, preferred_element_type=jnp.float32)


def prep_kernel(s_ref, x_hbm, ids_hbm, w_hbm, *refs):
    outs, (x_ref, ids_ref, w_ref, sems) = refs[:4], refs[4:]
    z, c = s_ref[0], s_ref[1]
    pairs = ((ids_hbm, ids_ref), (w_hbm, w_ref), (x_hbm, x_ref))
    copies = [pltpu.make_async_copy(a, b, sems.at[i]) for i, (a, b) in enumerate(pairs)]
    for copy in copies:
        copy.start()
    for copy in copies:
        copy.wait()
    w = w_ref[...]
    hi = w.astype(jnp.bfloat16)
    rest = w - hi.astype(jnp.float32)
    mid = rest.astype(jnp.bfloat16)
    low = (rest - mid.astype(jnp.float32)).astype(jnp.bfloat16)
    lane = lax.broadcasted_iota(jnp.int32, (TOP, EXT), 1)
    part = lax.broadcasted_iota(jnp.int32, (TOP, EXT), 0)
    ext = jnp.zeros((TOK, EXT), jnp.float32)
    for i, v in enumerate((ids_ref[...].astype(jnp.float32).astype(jnp.bfloat16), hi, mid, low)):
        spread = (lane == TOP * i + part).astype(jnp.bfloat16)
        ext = ext + lax.dot_general(v, spread, (((0,), (0,)), ((), ())), preferred_element_type=jnp.float32)
    ext = ext.astype(jnp.bfloat16)
    for j, out_ref in enumerate(outs):
        block = (z + 4 * c) % ZN if j == 0 else (z + ZN + jnp.where(c == 0, -j, j)) % ZN
        out_ref[...] = jnp.zeros((PADT, BLOCK + EXT), jnp.bfloat16)
        out_ref[:TOK, :BLOCK] = x_ref[:, pl.ds(pl.multiple_of(block * BLOCK, 128), BLOCK)]
        out_ref[:TOK, BLOCK:] = ext


def prep(s, x, ids, w):
    return pl.pallas_call(
        prep_kernel,
        out_shape=(jax.ShapeDtypeStruct((PADT, BLOCK + EXT), jnp.bfloat16),) * 4,
        in_specs=[SMEM] + [pl.BlockSpec(memory_space=pltpu.HBM)] * 3,
        out_specs=(VMEM,) * 4,
        scratch_shapes=[
            pltpu.VMEM((TOK, ZN * BLOCK), jnp.bfloat16),
            pltpu.VMEM((TOP, TOK), jnp.int32),
            pltpu.VMEM((TOP, TOK), jnp.float32),
            pltpu.SemaphoreType.DMA((3,)),
        ],
        compiler_params=PARAMS,
        name="prep",
    )(s, x, ids, w)


def pack_kernel(*refs):
    xs, (packed_ref, shared_ref, ext_ref) = refs[:4], refs[4:]
    n = 4 * PADT
    for i, x in enumerate(xs):
        shared_ref[i * PADT : (i + 1) * PADT] = x[:, :BLOCK]
        ext_ref[i * PADT : (i + 1) * PADT] = x[:, BLOCK:]
    x = shared_ref[...]
    ids = jnp.transpose(ext_ref[...].astype(jnp.float32))[:TOP, :].astype(jnp.int32)
    experts = lax.broadcasted_iota(jnp.int32, (EXPERTS, n), 0)
    row = lax.broadcasted_iota(jnp.int32, (EXPERTS, n), 1)
    member = jnp.zeros((EXPERTS, n), jnp.float32)
    for k in range(TOP):
        member = member + ((experts == ids[k : k + 1, :]) & (row % PADT < TOK)).astype(jnp.float32)
    r0 = lax.broadcasted_iota(jnp.int32, (n, n), 0)
    r1 = lax.broadcasted_iota(jnp.int32, (n, n), 1)
    before = ((r0 // PADT == r1 // PADT) & (r0 < r1)).astype(jnp.bfloat16)
    pos = fdot(member.astype(jnp.bfloat16), before).astype(jnp.int32)
    target = jnp.where(member > 0.5, row // PADT * CAP + pos, -1)
    wanted = lax.broadcasted_iota(jnp.int32, (4 * CAP, n), 0)
    for e in range(EXPERTS):
        pick = (wanted == target[e : e + 1, :]).astype(jnp.bfloat16)
        packed_ref[e] = fdot(pick, x).astype(jnp.bfloat16)


def pack(*xs):
    return pl.pallas_call(
        pack_kernel,
        out_shape=(
            jax.ShapeDtypeStruct((EXPERTS, 4 * CAP, BLOCK), jnp.bfloat16),
            jax.ShapeDtypeStruct((4 * PADT, BLOCK), jnp.bfloat16),
            jax.ShapeDtypeStruct((4 * PADT, EXT), jnp.bfloat16),
        ),
        in_specs=[VMEM] * 4,
        out_specs=(VMEM, VMEM, VMEM),
        compiler_params=PARAMS,
        name="pack",
    )(*xs)


def up_kernel(ks, c_ref, own_ref, oth_ref, so_ref, st_ref, wg_ref, wu_ref, sg_ref, su_ref, *refs):
    count = len(ks)
    out_refs, (x_ref, s_ref, full_ref) = refs[:-3], refs[-3:]

    def gather(sides):
        for at, k in enumerate(ks):
            side = 0 if k in HELD[0] else 1
            i = HELD[side].index(k)
            full, shared = sides[side]
            x_ref[at] = full[i]
            s_ref[at * PADT : (at + 1) * PADT] = shared[i * PADT : (i + 1) * PADT]

    own, oth = (own_ref, so_ref), (oth_ref, st_ref)
    start = pl.program_id(0) == 0

    @pl.when(start & (c_ref[0] == 0))
    def _():
        gather((own, oth))

    @pl.when(start & (c_ref[0] != 0))
    def _():
        gather((oth, own))

    for w_ref, v_ref, o_refs in ((wg_ref, sg_ref, out_refs[:count]), (wu_ref, su_ref, out_refs[count:])):
        shared = fdot(s_ref[...], v_ref[...]) * SCALE

        def chunk(i, carry):
            full_ref[i] = fdot(x_ref[i], w_ref[0]) * SCALE
            return carry

        lax.fori_loop(0, count, chunk, 0)
        for i in range(count):
            o_refs[i][:ROWS, :] = full_ref[i]
            o_refs[i][ROWS:, :] = shared[i * PADT : (i + 1) * PADT]


def up_dots(ks, c, own, oth, so, st, wg, wu, sg, su):
    whole = lambda *shape: pl.BlockSpec(shape, lambda n: (0,) * len(shape))
    count = len(ks)
    return pl.pallas_call(
        functools.partial(up_kernel, ks),
        grid=(FFH // NT,),
        out_shape=(jax.ShapeDtypeStruct((CHUNK, FFH), jnp.float32),) * (2 * count),
        in_specs=[
            SMEM,
            whole(4, ROWS, BLOCK),
            whole(4, ROWS, BLOCK),
            whole(4 * PADT, BLOCK),
            whole(4 * PADT, BLOCK),
            pl.BlockSpec((1, BLOCK, NT), lambda n: (0, 0, n)),
            pl.BlockSpec((1, BLOCK, NT), lambda n: (0, 0, n)),
            pl.BlockSpec((BLOCK, NT), lambda n: (0, n)),
            pl.BlockSpec((BLOCK, NT), lambda n: (0, n)),
        ],
        out_specs=(pl.BlockSpec((CHUNK, NT), lambda n: (0, n)),) * (2 * count),
        scratch_shapes=[
            pltpu.VMEM((count, ROWS, BLOCK), jnp.bfloat16),
            pltpu.VMEM((count * PADT, BLOCK), jnp.bfloat16),
            pltpu.VMEM((count, ROWS, NT), jnp.float32),
        ],
        compiler_params=PARAMS,
        cost_estimate=pl.CostEstimate(
            flops=2 * 2 * count * CHUNK * BLOCK * FFH, bytes_accessed=4 * BLOCK * FFH * 2, transcendentals=0
        ),
    )(c, own, oth, so, st, wg, wu, sg, su)


def down_kernel(c_ref, *refs):
    xs, (wd_ref, sd_ref, keep_ref, send_ref, x_ref, s_ref, full_ref) = refs[:-7], refs[-7:]
    n = len(xs) // 4
    for i in range(2 * n):
        for x, cols in zip(xs[2 * i : 2 * i + 2], (slice(0, CUT), slice(CUT, FFH))):
            x_ref[i, :, cols] = x[:ROWS]
            s_ref[i * PADT : (i + 1) * PADT, cols] = x[ROWS:]

    def chunk(i, carry):
        full_ref[i, :ROWS] = fdot(x_ref[i], wd_ref[0])
        return carry

    lax.fori_loop(0, 2 * n, chunk, 0)
    shared = fdot(s_ref[...], sd_ref[...])
    for i in range(2 * n):
        full_ref[i, ROWS:] = shared[i * PADT : (i + 1) * PADT]
    c = c_ref[0]
    for i in range(n):
        keep_ref[i] = full_ref[c * n + i]
        send_ref[i] = full_ref[(1 - c) * n + i]


def down_dots(c, xs, wd, sd):
    n = len(xs) // 4
    return pl.pallas_call(
        down_kernel,
        out_shape=(
            jax.ShapeDtypeStruct((n, CHUNK, BLOCK), jnp.float32),
            jax.ShapeDtypeStruct((n, CHUNK, BLOCK), jnp.float32),
        ),
        in_specs=[SMEM] + [VMEM] * (len(xs) + 2),
        out_specs=(VMEM, VMEM),
        scratch_shapes=[
            pltpu.VMEM((2 * n, ROWS, FFH), jnp.bfloat16),
            pltpu.VMEM((2 * n * PADT, FFH), jnp.bfloat16),
            pltpu.VMEM((2 * n, CHUNK, BLOCK), jnp.float32),
        ],
        compiler_params=PARAMS,
        cost_estimate=pl.CostEstimate(
            flops=2 * 2 * n * CHUNK * BLOCK * FFH, bytes_accessed=2 * BLOCK * FFH * 2, transcendentals=0
        ),
        name="down_dots",
    )(c, *xs, wd, sd)


def settle_kernel(keep_ref, came_ref, *refs):
    before, (rows_ref, shared_ref) = refs[:-2], refs[-2:]
    at = 0
    if before:
        at = 2 * CAP
        rows_ref[:, :at, :] = before[0][...]
    for i in range(2):
        total = keep_ref[i, :ROWS] + came_ref[i, :ROWS]
        rows_ref[:, at + i * CAP : at + (i + 1) * CAP, :] = total.reshape(EXPERTS, CAP, BLOCK).astype(jnp.bfloat16)
        shared_ref[i * PADT : (i + 1) * PADT] = keep_ref[i, ROWS:] + came_ref[i, ROWS:]


def settle(keep, came, *before):
    return pl.pallas_call(
        settle_kernel,
        out_shape=(
            jax.ShapeDtypeStruct((EXPERTS, (2 + 2 * len(before)) * CAP, BLOCK), jnp.bfloat16),
            jax.ShapeDtypeStruct((2 * PADT, BLOCK), jnp.float32),
        ),
        in_specs=[VMEM] * (2 + len(before)),
        out_specs=(VMEM, VMEM),
        compiler_params=PARAMS,
        name="settle",
    )(keep, came, *before)


def combine_kernel(ext_ref, back_ref, near_ref, far_ref, out_ref, terms_ref, total_ref):
    rows = 4 * PADT
    cols = 4 * ROWS
    ext = jnp.concatenate([ext_ref[PADT:], ext_ref[:PADT]], axis=0).astype(jnp.float32)
    weight = (ext[:, TOP : 2 * TOP] + ext[:, 2 * TOP : 3 * TOP]) + ext[:, 3 * TOP : 4 * TOP]
    column = lax.broadcasted_iota(jnp.int32, (rows, cols), 1)
    row = lax.broadcasted_iota(jnp.int32, (rows, cols), 0)
    live = (row % PADT < TOK) & (row // PADT == (column // CAP) % 4)
    owner = (column // (4 * CAP)).astype(jnp.float32)
    slot = (column % CAP).astype(jnp.float32)
    member = jnp.zeros((rows, cols), jnp.float32)
    scale = jnp.zeros((rows, cols), jnp.float32)
    for k in range(TOP):
        hit = (ext[:, k : k + 1] == owner) & live
        member = jnp.where(hit, 1.0, member)
        scale = jnp.where(hit, weight[:, k : k + 1], scale)
    i0 = lax.broadcasted_iota(jnp.int32, (rows, rows), 0)
    i1 = lax.broadcasted_iota(jnp.int32, (rows, rows), 1)
    before = ((i1 < i0) & (i0 // PADT == i1 // PADT)).astype(jnp.bfloat16)
    pos = fdot(before, member.astype(jnp.bfloat16))
    scale = jnp.where((pos == slot) & (member > 0.5), scale, 0.0)
    hi = scale.astype(jnp.bfloat16)
    rest = scale - hi.astype(jnp.float32)
    mid = rest.astype(jnp.bfloat16)
    low = (rest - mid.astype(jnp.float32)).astype(jnp.bfloat16)
    for i, term in enumerate((low, mid, hi)):
        terms_ref[i] = term
    total_ref[: 2 * PADT] = near_ref[...]
    total_ref[2 * PADT :] = far_ref[...]

    def add(i, carry):
        total_ref[...] += fdot(terms_ref[i], back_ref[...])
        return carry

    lax.fori_loop(0, 3, add, 0)
    out_ref[...] = total_ref[...].astype(jnp.bfloat16)


def combine(ext, back, near, far):
    return pl.pallas_call(
        combine_kernel,
        out_shape=jax.ShapeDtypeStruct((4 * PADT, BLOCK), jnp.bfloat16),
        in_specs=[VMEM, VMEM, VMEM, VMEM],
        out_specs=VMEM,
        scratch_shapes=[
            pltpu.VMEM((3, 4 * PADT, 4 * ROWS), jnp.bfloat16),
            pltpu.VMEM((4 * PADT, BLOCK), jnp.float32),
        ],
        compiler_params=PARAMS,
        name="combine",
    )(ext, back, near, far)


def assemble_kernel(s_ref, *refs):
    out_ref = refs[-1]
    z = s_ref[0]
    held_ref, came_ref = refs[:-1]
    a1, a2, b3, b0 = [held_ref[i * PADT : i * PADT + TOK] for i in range(4)]
    o1, o2, o3, o0 = [came_ref[i * PADT : i * PADT + TOK] for i in range(4)]

    def put(parts):
        for i, part in enumerate(parts):
            at = pl.multiple_of(((z + i) % ZN) * BLOCK, 128)
            out_ref[:, pl.ds(at, BLOCK)] = part

    @pl.when(s_ref[1] == 0)
    def _():
        put((b0, o1, o2, o3, o0, b3, a2, a1))

    @pl.when(s_ref[1] != 0)
    def _():
        put((o0, a1, a2, b3, b0, o3, o2, o1))


def assemble(s, *parts):
    return pl.pallas_call(
        assemble_kernel,
        out_shape=jax.ShapeDtypeStruct((TOK, ZN * BLOCK), jnp.bfloat16),
        in_specs=[SMEM] + [VMEM] * len(parts),
        out_specs=VMEM,
        compiler_params=PARAMS,
        name="assemble",
    )(s, *parts)


def ring(parts, shift):
    total = None
    for mine in parts:
        total = mine if total is None else mine + total.astype(jnp.float32)
        total = lax.ppermute(total.astype(LINK), "dp", shifted(shift))
    return total.astype(jnp.float32)


def layer(tokens, ids, weights, wg, wu, wd, sg, su, sd):
    z = lax.axis_index("dp")
    c = lax.axis_index("tensor")
    c1, zc = c.reshape(1), jnp.stack([z, c])
    sent = prep(zc, tokens, ids.T, weights.T)
    came = []
    for j, piece in enumerate(sent):
        came.append(lax.ppermute(piece, ("dp", "tensor"), paired(-j, -j) if j else paired(0, 4)))
    packed, shared_own, ext = pack(*came)
    arrived = lax.all_to_all(packed, "expert", 0, 0, tiled=True)
    both = jnp.concatenate([arrived.reshape(4 * ROWS, BLOCK), shared_own])
    both = lax.ppermute(both, "tensor", SWAP)
    shared_oth = both[4 * ROWS :]
    own, oth = [
        jnp.moveaxis(a.reshape(EXPERTS, 4, CAP, BLOCK), 1, 0).reshape(4, ROWS, BLOCK)
        for a in (arrived, both[: 4 * ROWS])
    ]
    args = (c1, own, oth, shared_own, shared_oth, wg, wu, sg, su)
    early = up_dots(EARLY, *args)
    late = up_dots(LATE, *args)
    gate = dict(zip(EARLY + LATE, early[: len(EARLY)] + late[: len(LATE)]))
    up = dict(zip(EARLY + LATE, early[len(EARLY) :] + late[len(LATE) :]))
    g_down = ring([gate[k] for k in (4, 3, 2, 1)], -1)
    u_up = ring([up[k] for k in (4, 5, 6, 7)], 1)
    u_down = ring([up[k] for k in (3, 2, 1)], -1)
    g_up = ring([gate[k] for k in (5, 6, 7)], 1)
    g = (gate[0] + (g_down + g_up)) * (1.0 / SCALE)
    u = (up[0] + (u_down + u_up)) * (1.0 / SCALE)
    hidden = (jax.nn.silu(g) * u).astype(jnp.bfloat16)
    top, tail = hidden[:, :CUT], hidden[:, CUT:]
    got = {0: (top, tail)}
    pd, pu, qd, qu = top, top, tail, tail
    for j in range(1, 5):
        pd = lax.ppermute(pd, "dp", shifted(-1))
        qu = lax.ppermute(qu, "dp", shifted(1))
        if j < 4:
            qd = lax.ppermute(qd, "dp", shifted(-1))
            pu = lax.ppermute(pu, "dp", shifted(1))
            got[ZN - j], got[j] = (pd, qd), (pu, qu)
        else:
            got[4] = (pd, qu)
    rows, shares = (), []
    for a, b in (((7, 6), (1, 2)), ((5, 0), (3, 4))):
        keep, send = down_dots(c1, [p for k in a + b for p in got[k]], wd, sd)
        came = lax.ppermute(send, "tensor", SWAP)
        *rows, shared = settle(keep, came, *rows)
        shares.append(shared)
    back = lax.all_to_all(rows[0], "expert", 0, 0, tiled=True).reshape(4 * ROWS, BLOCK)
    mixed = combine(ext, back, *shares)
    held = []
    for i, (to, fro) in enumerate(((1, 1), (2, 2), (3, 3), (0, 4))):
        held.append(lax.ppermute(mixed[i * PADT : (i + 1) * PADT], ("dp", "tensor"), paired(to, fro)))
    held = jnp.concatenate(held)
    others = lax.ppermute(held, "tensor", SWAP)
    return assemble(zc, held, others)


def solution(mesh):
    placed = (
        P(("dp", "expert"), None),
        P(("dp", "expert"), None),
        P(("dp", "expert"), None),
        P("expert", "dp", "tensor"),
        P("expert", "dp", "tensor"),
        P("expert", "tensor", "dp"),
        P("dp", "tensor"),
        P("dp", "tensor"),
        P("tensor", "dp"),
    )
    return jax.shard_map(layer, mesh=mesh, in_specs=placed, out_specs=P(("dp", "expert"), None), check_vma=False)
```

```python
import functools

import jax
import jax.numpy as jnp
from jax import lax
from jax.experimental import pallas as pl
from jax.experimental.pallas import tpu as pltpu
from jax.sharding import PartitionSpec as P

EXPERTS = 16
CAP = 8
TOP = 8
ZN = 8
TOK = 12
PADT = 16
BLOCK = 896
ROWS = EXPERTS * CAP
CHUNK = ROWS + PADT
FFH = 1024
CUT = FFH // 2
NT = 256
EXT = 128
HELD = ((0, 7, 6, 5), (4, 1, 2, 3))
EARLY = (3, 4, 5)
LATE = (6, 7, 0, 1, 2)
SCALE = 16.0
LINK = jnp.float16

PARAMS = pltpu.CompilerParams(vmem_limit_bytes=16 * 1024 * 1024)
VMEM = pl.BlockSpec(memory_space=pltpu.VMEM)
SMEM = pl.BlockSpec(memory_space=pltpu.SMEM)
SWAP = [(0, 1), (1, 0)]


def shifted(k):
    return [(i, (i + k) % ZN) for i in range(ZN)]


def paired(up, down):
    out = []
    for i in range(ZN):
        out.append((i * 2, ((i + up) % ZN) * 2))
        out.append((i * 2 + 1, ((i - down) % ZN) * 2 + 1))
    return out


def fdot(a, b):
    return jnp.dot(a, b, preferred_element_type=jnp.float32)


def prep_kernel(s_ref, x_hbm, ids_hbm, w_hbm, *refs):
    outs, (x_ref, ids_ref, w_ref, sems) = refs[:4], refs[4:]
    z, c = s_ref[0], s_ref[1]
    pairs = ((ids_hbm, ids_ref), (w_hbm, w_ref), (x_hbm, x_ref))
    copies = [pltpu.make_async_copy(a, b, sems.at[i]) for i, (a, b) in enumerate(pairs)]
    for copy in copies:
        copy.start()
    for copy in copies:
        copy.wait()
    w = w_ref[...]
    hi = w.astype(jnp.bfloat16)
    rest = w - hi.astype(jnp.float32)
    mid = rest.astype(jnp.bfloat16)
    low = (rest - mid.astype(jnp.float32)).astype(jnp.bfloat16)
    lane = lax.broadcasted_iota(jnp.int32, (TOP, EXT), 1)
    part = lax.broadcasted_iota(jnp.int32, (TOP, EXT), 0)
    ext = jnp.zeros((TOK, EXT), jnp.float32)
    for i, v in enumerate((ids_ref[...].astype(jnp.float32).astype(jnp.bfloat16), hi, mid, low)):
        spread = (lane == TOP * i + part).astype(jnp.bfloat16)
        ext = ext + lax.dot_general(v, spread, (((0,), (0,)), ((), ())), preferred_element_type=jnp.float32)
    ext = ext.astype(jnp.bfloat16)
    for j, out_ref in enumerate(outs):
        block = (z + 4 * c) % ZN if j == 0 else (z + ZN + jnp.where(c == 0, -j, j)) % ZN
        out_ref[...] = jnp.zeros((PADT, BLOCK + EXT), jnp.bfloat16)
        out_ref[:TOK, :BLOCK] = x_ref[:, pl.ds(pl.multiple_of(block * BLOCK, 128), BLOCK)]
        out_ref[:TOK, BLOCK:] = ext


def prep(s, x, ids, w):
    return pl.pallas_call(
        prep_kernel,
        out_shape=(jax.ShapeDtypeStruct((PADT, BLOCK + EXT), jnp.bfloat16),) * 4,
        in_specs=[SMEM] + [pl.BlockSpec(memory_space=pltpu.HBM)] * 3,
        out_specs=(VMEM,) * 4,
        scratch_shapes=[
            pltpu.VMEM((TOK, ZN * BLOCK), jnp.bfloat16),
            pltpu.VMEM((TOP, TOK), jnp.int32),
            pltpu.VMEM((TOP, TOK), jnp.float32),
            pltpu.SemaphoreType.DMA((3,)),
        ],
        compiler_params=PARAMS,
        name="prep",
    )(s, x, ids, w)


def pack_kernel(*refs):
    xs, (packed_ref, shared_ref, ext_ref) = refs[:4], refs[4:]
    n = 4 * PADT
    for i, x in enumerate(xs):
        shared_ref[i * PADT : (i + 1) * PADT] = x[:, :BLOCK]
        ext_ref[i * PADT : (i + 1) * PADT] = x[:, BLOCK:]
    x = shared_ref[...]
    ids = jnp.transpose(ext_ref[...].astype(jnp.float32))[:TOP, :].astype(jnp.int32)
    experts = lax.broadcasted_iota(jnp.int32, (EXPERTS, n), 0)
    row = lax.broadcasted_iota(jnp.int32, (EXPERTS, n), 1)
    member = jnp.zeros((EXPERTS, n), jnp.float32)
    for k in range(TOP):
        member = member + ((experts == ids[k : k + 1, :]) & (row % PADT < TOK)).astype(jnp.float32)
    r0 = lax.broadcasted_iota(jnp.int32, (n, n), 0)
    r1 = lax.broadcasted_iota(jnp.int32, (n, n), 1)
    before = ((r0 // PADT == r1 // PADT) & (r0 < r1)).astype(jnp.bfloat16)
    pos = fdot(member.astype(jnp.bfloat16), before).astype(jnp.int32)
    target = jnp.where(member > 0.5, row // PADT * CAP + pos, -1)
    wanted = lax.broadcasted_iota(jnp.int32, (4 * CAP, n), 0)
    for e in range(EXPERTS):
        pick = (wanted == target[e : e + 1, :]).astype(jnp.bfloat16)
        packed_ref[e] = fdot(pick, x).astype(jnp.bfloat16)


def pack(*xs):
    return pl.pallas_call(
        pack_kernel,
        out_shape=(
            jax.ShapeDtypeStruct((EXPERTS, 4 * CAP, BLOCK), jnp.bfloat16),
            jax.ShapeDtypeStruct((4 * PADT, BLOCK), jnp.bfloat16),
            jax.ShapeDtypeStruct((4 * PADT, EXT), jnp.bfloat16),
        ),
        in_specs=[VMEM] * 4,
        out_specs=(VMEM, VMEM, VMEM),
        compiler_params=PARAMS,
        name="pack",
    )(*xs)


def up_kernel(ks, c_ref, own_ref, oth_ref, so_ref, st_ref, wg_ref, wu_ref, sg_ref, su_ref, *refs):
    count = len(ks)
    out_refs, (x_ref, s_ref, full_ref) = refs[:-3], refs[-3:]

    def gather(sides):
        for at, k in enumerate(ks):
            side = 0 if k in HELD[0] else 1
            i = HELD[side].index(k)
            full, shared = sides[side]
            x_ref[at * ROWS : (at + 1) * ROWS] = full[i]
            s_ref[at * PADT : (at + 1) * PADT] = shared[i * PADT : (i + 1) * PADT]

    own, oth = (own_ref, so_ref), (oth_ref, st_ref)
    start = pl.program_id(0) == 0

    @pl.when(start & (c_ref[0] == 0))
    def _():
        gather((own, oth))

    @pl.when(start & (c_ref[0] != 0))
    def _():
        gather((oth, own))

    for w_ref, v_ref, o_refs in ((wg_ref, sg_ref, out_refs[:count]), (wu_ref, su_ref, out_refs[count:])):
        shared = fdot(s_ref[...], v_ref[...]) * SCALE
        if count == len(EARLY):
            full_ref[...] = fdot(x_ref[...], w_ref[0]) * SCALE
        else:
            half = count * ROWS // 2

            def part(i, carry):
                rows = pl.ds(pl.multiple_of(i * half, half), half)
                full_ref[rows, :] = fdot(x_ref[rows, :], w_ref[0]) * SCALE
                return carry

            lax.fori_loop(0, 2, part, 0)
        for i in range(count):
            o_refs[i][:ROWS, :] = full_ref[i * ROWS : (i + 1) * ROWS]
            o_refs[i][ROWS:, :] = shared[i * PADT : (i + 1) * PADT]


def up_dots(ks, c, own, oth, so, st, wg, wu, sg, su):
    whole = lambda *shape: pl.BlockSpec(shape, lambda n: (0,) * len(shape))
    count = len(ks)
    return pl.pallas_call(
        functools.partial(up_kernel, ks),
        grid=(FFH // NT,),
        out_shape=(jax.ShapeDtypeStruct((CHUNK, FFH), jnp.float32),) * (2 * count),
        in_specs=[
            SMEM,
            whole(4, ROWS, BLOCK),
            whole(4, ROWS, BLOCK),
            whole(4 * PADT, BLOCK),
            whole(4 * PADT, BLOCK),
            pl.BlockSpec((1, BLOCK, NT), lambda n: (0, 0, n)),
            pl.BlockSpec((1, BLOCK, NT), lambda n: (0, 0, n)),
            pl.BlockSpec((BLOCK, NT), lambda n: (0, n)),
            pl.BlockSpec((BLOCK, NT), lambda n: (0, n)),
        ],
        out_specs=(pl.BlockSpec((CHUNK, NT), lambda n: (0, n)),) * (2 * count),
        scratch_shapes=[
            pltpu.VMEM((count * ROWS, BLOCK), jnp.bfloat16),
            pltpu.VMEM((count * PADT, BLOCK), jnp.bfloat16),
            pltpu.VMEM((count * ROWS, NT), jnp.float32),
        ],
        compiler_params=PARAMS,
        cost_estimate=pl.CostEstimate(
            flops=2 * 2 * count * CHUNK * BLOCK * FFH, bytes_accessed=4 * BLOCK * FFH * 2, transcendentals=0
        ),
    )(c, own, oth, so, st, wg, wu, sg, su)


def down_kernel(c_ref, *refs):
    xs, (wd_ref, sd_ref, keep_ref, send_ref, x_ref, s_ref, full_ref) = refs[:-7], refs[-7:]
    n = len(xs) // 4
    for i in range(2 * n):
        for x, cols in zip(xs[2 * i : 2 * i + 2], (slice(0, CUT), slice(CUT, FFH))):
            x_ref[i, :, cols] = x[:ROWS]
            s_ref[i * PADT : (i + 1) * PADT, cols] = x[ROWS:]

    def chunk(i, carry):
        full_ref[i, :ROWS] = fdot(x_ref[i], wd_ref[0])
        return carry

    lax.fori_loop(0, 2 * n, chunk, 0)
    shared = fdot(s_ref[...], sd_ref[...])
    for i in range(2 * n):
        full_ref[i, ROWS:] = shared[i * PADT : (i + 1) * PADT]
    c = c_ref[0]
    for i in range(n):
        keep_ref[i] = full_ref[c * n + i]
        send_ref[i] = full_ref[(1 - c) * n + i]


def down_dots(c, xs, wd, sd):
    n = len(xs) // 4
    return pl.pallas_call(
        down_kernel,
        out_shape=(
            jax.ShapeDtypeStruct((n, CHUNK, BLOCK), jnp.float32),
            jax.ShapeDtypeStruct((n, CHUNK, BLOCK), jnp.float32),
        ),
        in_specs=[SMEM] + [VMEM] * (len(xs) + 2),
        out_specs=(VMEM, VMEM),
        scratch_shapes=[
            pltpu.VMEM((2 * n, ROWS, FFH), jnp.bfloat16),
            pltpu.VMEM((2 * n * PADT, FFH), jnp.bfloat16),
            pltpu.VMEM((2 * n, CHUNK, BLOCK), jnp.float32),
        ],
        compiler_params=PARAMS,
        cost_estimate=pl.CostEstimate(
            flops=2 * 2 * n * CHUNK * BLOCK * FFH, bytes_accessed=2 * BLOCK * FFH * 2, transcendentals=0
        ),
        name="down_dots",
    )(c, *xs, wd, sd)


def settle_kernel(keep_ref, came_ref, *refs):
    before, (rows_ref, shared_ref) = refs[:-2], refs[-2:]
    at = 0
    if before:
        at = 2 * CAP
        rows_ref[:, :at, :] = before[0][...]
    for i in range(2):
        total = keep_ref[i, :ROWS] + came_ref[i, :ROWS]
        rows_ref[:, at + i * CAP : at + (i + 1) * CAP, :] = total.reshape(EXPERTS, CAP, BLOCK).astype(jnp.bfloat16)
        shared_ref[i * PADT : (i + 1) * PADT] = keep_ref[i, ROWS:] + came_ref[i, ROWS:]


def settle(keep, came, *before):
    return pl.pallas_call(
        settle_kernel,
        out_shape=(
            jax.ShapeDtypeStruct((EXPERTS, (2 + 2 * len(before)) * CAP, BLOCK), jnp.bfloat16),
            jax.ShapeDtypeStruct((2 * PADT, BLOCK), jnp.float32),
        ),
        in_specs=[VMEM] * (2 + len(before)),
        out_specs=(VMEM, VMEM),
        compiler_params=PARAMS,
        name="settle",
    )(keep, came, *before)


def combine_kernel(ext_ref, back_ref, near_ref, far_ref, out_ref, terms_ref, total_ref):
    rows = 4 * PADT
    cols = 4 * ROWS
    ext = jnp.concatenate([ext_ref[PADT:], ext_ref[:PADT]], axis=0).astype(jnp.float32)
    weight = (ext[:, TOP : 2 * TOP] + ext[:, 2 * TOP : 3 * TOP]) + ext[:, 3 * TOP : 4 * TOP]
    column = lax.broadcasted_iota(jnp.int32, (rows, cols), 1)
    row = lax.broadcasted_iota(jnp.int32, (rows, cols), 0)
    live = (row % PADT < TOK) & (row // PADT == (column // CAP) % 4)
    owner = (column // (4 * CAP)).astype(jnp.float32)
    slot = (column % CAP).astype(jnp.float32)
    member = jnp.zeros((rows, cols), jnp.float32)
    scale = jnp.zeros((rows, cols), jnp.float32)
    for k in range(TOP):
        hit = (ext[:, k : k + 1] == owner) & live
        member = jnp.where(hit, 1.0, member)
        scale = jnp.where(hit, weight[:, k : k + 1], scale)
    i0 = lax.broadcasted_iota(jnp.int32, (rows, rows), 0)
    i1 = lax.broadcasted_iota(jnp.int32, (rows, rows), 1)
    before = ((i1 < i0) & (i0 // PADT == i1 // PADT)).astype(jnp.bfloat16)
    pos = fdot(before, member.astype(jnp.bfloat16))
    scale = jnp.where((pos == slot) & (member > 0.5), scale, 0.0)
    hi = scale.astype(jnp.bfloat16)
    rest = scale - hi.astype(jnp.float32)
    mid = rest.astype(jnp.bfloat16)
    low = (rest - mid.astype(jnp.float32)).astype(jnp.bfloat16)
    for i, term in enumerate((low, mid, hi)):
        terms_ref[i] = term
    total_ref[: 2 * PADT] = near_ref[...]
    total_ref[2 * PADT :] = far_ref[...]

    def add(i, carry):
        total_ref[...] += fdot(terms_ref[i], back_ref[...])
        return carry

    lax.fori_loop(0, 3, add, 0)
    out_ref[...] = total_ref[...].astype(jnp.bfloat16)


def combine(ext, back, near, far):
    return pl.pallas_call(
        combine_kernel,
        out_shape=jax.ShapeDtypeStruct((4 * PADT, BLOCK), jnp.bfloat16),
        in_specs=[VMEM, VMEM, VMEM, VMEM],
        out_specs=VMEM,
        scratch_shapes=[
            pltpu.VMEM((3, 4 * PADT, 4 * ROWS), jnp.bfloat16),
            pltpu.VMEM((4 * PADT, BLOCK), jnp.float32),
        ],
        compiler_params=PARAMS,
        name="combine",
    )(ext, back, near, far)


def assemble_kernel(s_ref, *refs):
    out_ref = refs[-1]
    z = s_ref[0]
    held_ref, came_ref = refs[:-1]
    a1, a2, b3, b0 = [held_ref[i * PADT : i * PADT + TOK] for i in range(4)]
    o1, o2, o3, o0 = [came_ref[i * PADT : i * PADT + TOK] for i in range(4)]

    def put(parts):
        for i, part in enumerate(parts):
            at = pl.multiple_of(((z + i) % ZN) * BLOCK, 128)
            out_ref[:, pl.ds(at, BLOCK)] = part

    @pl.when(s_ref[1] == 0)
    def _():
        put((b0, o1, o2, o3, o0, b3, a2, a1))

    @pl.when(s_ref[1] != 0)
    def _():
        put((o0, a1, a2, b3, b0, o3, o2, o1))


def assemble(s, *parts):
    return pl.pallas_call(
        assemble_kernel,
        out_shape=jax.ShapeDtypeStruct((TOK, ZN * BLOCK), jnp.bfloat16),
        in_specs=[SMEM] + [VMEM] * len(parts),
        out_specs=VMEM,
        compiler_params=PARAMS,
        name="assemble",
    )(s, *parts)


def ring(parts, shift):
    total = None
    for mine in parts:
        total = mine if total is None else mine + total.astype(jnp.float32)
        total = lax.ppermute(total.astype(LINK), "dp", shifted(shift))
    return total.astype(jnp.float32)


def layer(tokens, ids, weights, wg, wu, wd, sg, su, sd):
    z = lax.axis_index("dp")
    c = lax.axis_index("tensor")
    c1, zc = c.reshape(1), jnp.stack([z, c])
    sent = prep(zc, tokens, ids.T, weights.T)
    came = []
    for j, piece in enumerate(sent):
        came.append(lax.ppermute(piece, ("dp", "tensor"), paired(-j, -j) if j else paired(0, 4)))
    packed, shared_own, ext = pack(*came)
    arrived = lax.all_to_all(packed, "expert", 0, 0, tiled=True)
    both = jnp.concatenate([arrived.reshape(4 * ROWS, BLOCK), shared_own])
    both = lax.ppermute(both, "tensor", SWAP)
    shared_oth = both[4 * ROWS :]
    own, oth = [
        jnp.moveaxis(a.reshape(EXPERTS, 4, CAP, BLOCK), 1, 0).reshape(4, ROWS, BLOCK)
        for a in (arrived, both[: 4 * ROWS])
    ]
    args = (c1, own, oth, shared_own, shared_oth, wg, wu, sg, su)
    early = up_dots(EARLY, *args)
    late = up_dots(LATE, *args)
    gate = dict(zip(EARLY + LATE, early[: len(EARLY)] + late[: len(LATE)]))
    up = dict(zip(EARLY + LATE, early[len(EARLY) :] + late[len(LATE) :]))
    g_down = ring([gate[k] for k in (4, 3, 2, 1)], -1)
    u_up = ring([up[k] for k in (4, 5, 6, 7)], 1)
    u_down = ring([up[k] for k in (3, 2, 1)], -1)
    g_up = ring([gate[k] for k in (5, 6, 7)], 1)
    g = (gate[0] + (g_down + g_up)) * (1.0 / SCALE)
    u = (up[0] + (u_down + u_up)) * (1.0 / SCALE)
    hidden = (jax.nn.silu(g) * u).astype(jnp.bfloat16)
    top, tail = hidden[:, :CUT], hidden[:, CUT:]
    got = {0: (top, tail)}
    pd, pu, qd, qu = top, top, tail, tail
    for j in range(1, 5):
        pd = lax.ppermute(pd, "dp", shifted(-1))
        qu = lax.ppermute(qu, "dp", shifted(1))
        if j < 4:
            qd = lax.ppermute(qd, "dp", shifted(-1))
            pu = lax.ppermute(pu, "dp", shifted(1))
            got[ZN - j], got[j] = (pd, qd), (pu, qu)
        else:
            got[4] = (pd, qu)
    rows, shares = (), []
    for a, b in (((7, 6), (1, 2)), ((5, 0), (3, 4))):
        keep, send = down_dots(c1, [p for k in a + b for p in got[k]], wd, sd)
        came = lax.ppermute(send, "tensor", SWAP)
        *rows, shared = settle(keep, came, *rows)
        shares.append(shared)
    back = lax.all_to_all(rows[0], "expert", 0, 0, tiled=True).reshape(4 * ROWS, BLOCK)
    mixed = combine(ext, back, *shares)
    held = []
    for i, (to, fro) in enumerate(((1, 1), (2, 2), (3, 3), (0, 4))):
        held.append(lax.ppermute(mixed[i * PADT : (i + 1) * PADT], ("dp", "tensor"), paired(to, fro)))
    held = jnp.concatenate(held)
    others = lax.ppermute(held, "tensor", SWAP)
    return assemble(zc, held, others)


def solution(mesh):
    placed = (
        P(("dp", "expert"), None),
        P(("dp", "expert"), None),
        P(("dp", "expert"), None),
        P("expert", "dp", "tensor"),
        P("expert", "dp", "tensor"),
        P("expert", "tensor", "dp"),
        P("dp", "tensor"),
        P("dp", "tensor"),
        P("tensor", "dp"),
    )
    return jax.shard_map(layer, mesh=mesh, in_specs=placed, out_specs=P(("dp", "expert"), None), check_vma=False)
```

```python
import functools

import jax
import jax.numpy as jnp
from jax import lax
from jax.experimental import pallas as pl
from jax.experimental.pallas import tpu as pltpu
from jax.sharding import PartitionSpec as P

EXPERTS = 16
CAP = 8
TOP = 8
ZN = 8
TOK = 12
PADT = 16
BLOCK = 896
ROWS = EXPERTS * CAP
CHUNK = ROWS + PADT
FFH = 1024
CUT = FFH // 2
NT = 256
EXT = 128
HELD = ((0, 7, 6, 5), (4, 1, 2, 3))
EARLY = (3, 4, 5)
LATE = (6, 7, 0, 1, 2)
SCALE = 16.0
LINK = jnp.float16

PARAMS = pltpu.CompilerParams(vmem_limit_bytes=16 * 1024 * 1024)
VMEM = pl.BlockSpec(memory_space=pltpu.VMEM)
SMEM = pl.BlockSpec(memory_space=pltpu.SMEM)
SWAP = [(0, 1), (1, 0)]


def shifted(k):
    return [(i, (i + k) % ZN) for i in range(ZN)]


def paired(up, down):
    out = []
    for i in range(ZN):
        out.append((i * 2, ((i + up) % ZN) * 2))
        out.append((i * 2 + 1, ((i - down) % ZN) * 2 + 1))
    return out


def fdot(a, b):
    return jnp.dot(a, b, preferred_element_type=jnp.float32)


def prep_kernel(s_ref, x_hbm, ids_hbm, w_hbm, *refs):
    outs, (x_ref, ids_ref, w_ref, sems) = refs[:4], refs[4:]
    z, c = s_ref[0], s_ref[1]
    pairs = ((ids_hbm, ids_ref), (w_hbm, w_ref), (x_hbm, x_ref))
    copies = [pltpu.make_async_copy(a, b, sems.at[i]) for i, (a, b) in enumerate(pairs)]
    for copy in copies:
        copy.start()
    for copy in copies:
        copy.wait()
    w = w_ref[...]
    hi = w.astype(jnp.bfloat16)
    rest = w - hi.astype(jnp.float32)
    mid = rest.astype(jnp.bfloat16)
    low = (rest - mid.astype(jnp.float32)).astype(jnp.bfloat16)
    lane = lax.broadcasted_iota(jnp.int32, (TOP, EXT), 1)
    part = lax.broadcasted_iota(jnp.int32, (TOP, EXT), 0)
    ext = jnp.zeros((TOK, EXT), jnp.float32)
    for i, v in enumerate((ids_ref[...].astype(jnp.float32).astype(jnp.bfloat16), hi, mid, low)):
        spread = (lane == TOP * i + part).astype(jnp.bfloat16)
        ext = ext + lax.dot_general(v, spread, (((0,), (0,)), ((), ())), preferred_element_type=jnp.float32)
    ext = ext.astype(jnp.bfloat16)
    for j, out_ref in enumerate(outs):
        block = (z + 4 * c) % ZN if j == 0 else (z + ZN + jnp.where(c == 0, -j, j)) % ZN
        out_ref[...] = jnp.zeros((PADT, BLOCK + EXT), jnp.bfloat16)
        out_ref[:TOK, :BLOCK] = x_ref[:, pl.ds(pl.multiple_of(block * BLOCK, 128), BLOCK)]
        out_ref[:TOK, BLOCK:] = ext


def prep(s, x, ids, w):
    return pl.pallas_call(
        prep_kernel,
        out_shape=(jax.ShapeDtypeStruct((PADT, BLOCK + EXT), jnp.bfloat16),) * 4,
        in_specs=[SMEM] + [pl.BlockSpec(memory_space=pltpu.HBM)] * 3,
        out_specs=(VMEM,) * 4,
        scratch_shapes=[
            pltpu.VMEM((TOK, ZN * BLOCK), jnp.bfloat16),
            pltpu.VMEM((TOP, TOK), jnp.int32),
            pltpu.VMEM((TOP, TOK), jnp.float32),
            pltpu.SemaphoreType.DMA((3,)),
        ],
        compiler_params=PARAMS,
        name="prep",
    )(s, x, ids, w)


def pack_kernel(*refs):
    xs, (packed_ref, shared_ref, ext_ref) = refs[:4], refs[4:]
    n = 4 * PADT
    for i, x in enumerate(xs):
        shared_ref[i * PADT : (i + 1) * PADT] = x[:, :BLOCK]
        ext_ref[i * PADT : (i + 1) * PADT] = x[:, BLOCK:]
    x = shared_ref[...]
    ids = jnp.transpose(ext_ref[...].astype(jnp.float32))[:TOP, :].astype(jnp.int32)
    experts = lax.broadcasted_iota(jnp.int32, (EXPERTS, n), 0)
    row = lax.broadcasted_iota(jnp.int32, (EXPERTS, n), 1)
    member = jnp.zeros((EXPERTS, n), jnp.float32)
    for k in range(TOP):
        member = member + ((experts == ids[k : k + 1, :]) & (row % PADT < TOK)).astype(jnp.float32)
    r0 = lax.broadcasted_iota(jnp.int32, (n, n), 0)
    r1 = lax.broadcasted_iota(jnp.int32, (n, n), 1)
    before = ((r0 // PADT == r1 // PADT) & (r0 < r1)).astype(jnp.bfloat16)
    pos = fdot(member.astype(jnp.bfloat16), before).astype(jnp.int32)
    target = jnp.where(member > 0.5, row // PADT * CAP + pos, -1)
    wanted = lax.broadcasted_iota(jnp.int32, (4 * CAP, n), 0)
    for e in range(EXPERTS):
        pick = (wanted == target[e : e + 1, :]).astype(jnp.bfloat16)
        packed_ref[e] = fdot(pick, x).astype(jnp.bfloat16)


def pack(*xs):
    return pl.pallas_call(
        pack_kernel,
        out_shape=(
            jax.ShapeDtypeStruct((EXPERTS, 4 * CAP, BLOCK), jnp.bfloat16),
            jax.ShapeDtypeStruct((4 * PADT, BLOCK), jnp.bfloat16),
            jax.ShapeDtypeStruct((4 * PADT, EXT), jnp.bfloat16),
        ),
        in_specs=[VMEM] * 4,
        out_specs=(VMEM, VMEM, VMEM),
        compiler_params=PARAMS,
        name="pack",
    )(*xs)


def up_kernel(ks, c_ref, own_ref, oth_ref, so_ref, st_ref, wg_ref, wu_ref, sg_ref, su_ref, *refs):
    count = len(ks)
    out_refs, (x_ref, s_ref, full_ref) = refs[:-3], refs[-3:]

    def gather(sides):
        for at, k in enumerate(ks):
            side = 0 if k in HELD[0] else 1
            i = HELD[side].index(k)
            full, shared = sides[side]
            x_ref[at * ROWS : (at + 1) * ROWS] = full[i]
            s_ref[at * PADT : (at + 1) * PADT] = shared[i * PADT : (i + 1) * PADT]

    own, oth = (own_ref, so_ref), (oth_ref, st_ref)
    start = pl.program_id(0) == 0

    @pl.when(start & (c_ref[0] == 0))
    def _():
        gather((own, oth))

    @pl.when(start & (c_ref[0] != 0))
    def _():
        gather((oth, own))

    for w_ref, v_ref, o_refs in ((wg_ref, sg_ref, out_refs[:count]), (wu_ref, su_ref, out_refs[count:])):
        shared = fdot(s_ref[...], v_ref[...]) * SCALE
        full_ref[...] = fdot(x_ref[...], w_ref[0]) * SCALE
        for i in range(count):
            o_refs[i][:ROWS, :] = full_ref[i * ROWS : (i + 1) * ROWS]
            o_refs[i][ROWS:, :] = shared[i * PADT : (i + 1) * PADT]


def up_dots(ks, c, own, oth, so, st, wg, wu, sg, su):
    whole = lambda *shape: pl.BlockSpec(shape, lambda n: (0,) * len(shape))
    count = len(ks)
    return pl.pallas_call(
        functools.partial(up_kernel, ks),
        grid=(FFH // NT,),
        out_shape=(jax.ShapeDtypeStruct((CHUNK, FFH), jnp.float32),) * (2 * count),
        in_specs=[
            SMEM,
            whole(4, ROWS, BLOCK),
            whole(4, ROWS, BLOCK),
            whole(4 * PADT, BLOCK),
            whole(4 * PADT, BLOCK),
            pl.BlockSpec((1, BLOCK, NT), lambda n: (0, 0, n)),
            pl.BlockSpec((1, BLOCK, NT), lambda n: (0, 0, n)),
            pl.BlockSpec((BLOCK, NT), lambda n: (0, n)),
            pl.BlockSpec((BLOCK, NT), lambda n: (0, n)),
        ],
        out_specs=(pl.BlockSpec((CHUNK, NT), lambda n: (0, n)),) * (2 * count),
        scratch_shapes=[
            pltpu.VMEM((count * ROWS, BLOCK), jnp.bfloat16),
            pltpu.VMEM((count * PADT, BLOCK), jnp.bfloat16),
            pltpu.VMEM((count * ROWS, NT), jnp.float32),
        ],
        compiler_params=PARAMS,
        cost_estimate=pl.CostEstimate(
            flops=2 * 2 * count * CHUNK * BLOCK * FFH, bytes_accessed=4 * BLOCK * FFH * 2, transcendentals=0
        ),
    )(c, own, oth, so, st, wg, wu, sg, su)


def down_kernel(c_ref, *refs):
    xs, (wd_ref, sd_ref, keep_ref, send_ref, x_ref, s_ref, full_ref) = refs[:-7], refs[-7:]
    n = len(xs) // 4
    for i in range(2 * n):
        for x, cols in zip(xs[2 * i : 2 * i + 2], (slice(0, CUT), slice(CUT, FFH))):
            x_ref[i, :, cols] = x[:ROWS]
            s_ref[i * PADT : (i + 1) * PADT, cols] = x[ROWS:]

    def chunk(i, carry):
        full_ref[i, :ROWS] = fdot(x_ref[i], wd_ref[0])
        return carry

    lax.fori_loop(0, 2 * n, chunk, 0)
    shared = fdot(s_ref[...], sd_ref[...])
    for i in range(2 * n):
        full_ref[i, ROWS:] = shared[i * PADT : (i + 1) * PADT]
    c = c_ref[0]
    for i in range(n):
        keep_ref[i] = full_ref[c * n + i]
        send_ref[i] = full_ref[(1 - c) * n + i]


def down_dots(c, xs, wd, sd):
    n = len(xs) // 4
    return pl.pallas_call(
        down_kernel,
        out_shape=(
            jax.ShapeDtypeStruct((n, CHUNK, BLOCK), jnp.float32),
            jax.ShapeDtypeStruct((n, CHUNK, BLOCK), jnp.float32),
        ),
        in_specs=[SMEM] + [VMEM] * (len(xs) + 2),
        out_specs=(VMEM, VMEM),
        scratch_shapes=[
            pltpu.VMEM((2 * n, ROWS, FFH), jnp.bfloat16),
            pltpu.VMEM((2 * n * PADT, FFH), jnp.bfloat16),
            pltpu.VMEM((2 * n, CHUNK, BLOCK), jnp.float32),
        ],
        compiler_params=PARAMS,
        cost_estimate=pl.CostEstimate(
            flops=2 * 2 * n * CHUNK * BLOCK * FFH, bytes_accessed=2 * BLOCK * FFH * 2, transcendentals=0
        ),
        name="down_dots",
    )(c, *xs, wd, sd)


def settle_kernel(near_ref, far_ref, came_ref, rows_ref, shared_ref):
    for i in range(4):
        keep = (near_ref, far_ref)[i // 2]
        total = keep[i % 2, :ROWS] + came_ref[i, :ROWS]
        rows_ref[:, i * CAP : (i + 1) * CAP, :] = total.reshape(EXPERTS, CAP, BLOCK).astype(jnp.bfloat16)
        shared_ref[i * PADT : (i + 1) * PADT] = keep[i % 2, ROWS:] + came_ref[i, ROWS:]


def settle(near, far, came):
    return pl.pallas_call(
        settle_kernel,
        out_shape=(
            jax.ShapeDtypeStruct((EXPERTS, 4 * CAP, BLOCK), jnp.bfloat16),
            jax.ShapeDtypeStruct((4 * PADT, BLOCK), jnp.float32),
        ),
        in_specs=[VMEM] * 3,
        out_specs=(VMEM, VMEM),
        compiler_params=PARAMS,
        name="settle",
    )(near, far, came)


def combine_kernel(ext_ref, back_ref, shared_ref, out_ref, terms_ref, total_ref):
    rows = 4 * PADT
    cols = 4 * ROWS
    ext = jnp.concatenate([ext_ref[PADT:], ext_ref[:PADT]], axis=0).astype(jnp.float32)
    weight = (ext[:, TOP : 2 * TOP] + ext[:, 2 * TOP : 3 * TOP]) + ext[:, 3 * TOP : 4 * TOP]
    column = lax.broadcasted_iota(jnp.int32, (rows, cols), 1)
    row = lax.broadcasted_iota(jnp.int32, (rows, cols), 0)
    live = (row % PADT < TOK) & (row // PADT == (column // CAP) % 4)
    owner = (column // (4 * CAP)).astype(jnp.float32)
    slot = (column % CAP).astype(jnp.float32)
    member = jnp.zeros((rows, cols), jnp.float32)
    scale = jnp.zeros((rows, cols), jnp.float32)
    for k in range(TOP):
        hit = (ext[:, k : k + 1] == owner) & live
        member = jnp.where(hit, 1.0, member)
        scale = jnp.where(hit, weight[:, k : k + 1], scale)
    i0 = lax.broadcasted_iota(jnp.int32, (rows, rows), 0)
    i1 = lax.broadcasted_iota(jnp.int32, (rows, rows), 1)
    before = ((i1 < i0) & (i0 // PADT == i1 // PADT)).astype(jnp.bfloat16)
    pos = fdot(before, member.astype(jnp.bfloat16))
    scale = jnp.where((pos == slot) & (member > 0.5), scale, 0.0)
    hi = scale.astype(jnp.bfloat16)
    rest = scale - hi.astype(jnp.float32)
    mid = rest.astype(jnp.bfloat16)
    low = (rest - mid.astype(jnp.float32)).astype(jnp.bfloat16)
    for i, term in enumerate((low, mid, hi)):
        terms_ref[i] = term
    total_ref[...] = shared_ref[...]

    def add(i, carry):
        total_ref[...] += fdot(terms_ref[i], back_ref[...])
        return carry

    lax.fori_loop(0, 3, add, 0)
    out_ref[...] = total_ref[...].astype(jnp.bfloat16)


def combine(ext, back, shared):
    return pl.pallas_call(
        combine_kernel,
        out_shape=jax.ShapeDtypeStruct((4 * PADT, BLOCK), jnp.bfloat16),
        in_specs=[VMEM, VMEM, VMEM],
        out_specs=VMEM,
        scratch_shapes=[
            pltpu.VMEM((3, 4 * PADT, 4 * ROWS), jnp.bfloat16),
            pltpu.VMEM((4 * PADT, BLOCK), jnp.float32),
        ],
        compiler_params=PARAMS,
        name="combine",
    )(ext, back, shared)


def assemble_kernel(s_ref, *refs):
    out_ref = refs[-1]
    z = s_ref[0]
    held_ref, came_ref = refs[:-1]
    a1, a2, b3, b0 = [held_ref[i * PADT : i * PADT + TOK] for i in range(4)]
    o1, o2, o3, o0 = [came_ref[i * PADT : i * PADT + TOK] for i in range(4)]

    def put(parts):
        for i, part in enumerate(parts):
            at = pl.multiple_of(((z + i) % ZN) * BLOCK, 128)
            out_ref[:, pl.ds(at, BLOCK)] = part

    @pl.when(s_ref[1] == 0)
    def _():
        put((b0, o1, o2, o3, o0, b3, a2, a1))

    @pl.when(s_ref[1] != 0)
    def _():
        put((o0, a1, a2, b3, b0, o3, o2, o1))


def assemble(s, *parts):
    return pl.pallas_call(
        assemble_kernel,
        out_shape=jax.ShapeDtypeStruct((TOK, ZN * BLOCK), jnp.bfloat16),
        in_specs=[SMEM] + [VMEM] * len(parts),
        out_specs=VMEM,
        compiler_params=PARAMS,
        name="assemble",
    )(s, *parts)


def ring(parts, shift):
    total = None
    for mine in parts:
        total = mine if total is None else mine + total.astype(jnp.float32)
        total = lax.ppermute(total.astype(LINK), "dp", shifted(shift))
    return total.astype(jnp.float32)


def layer(tokens, ids, weights, wg, wu, wd, sg, su, sd):
    z = lax.axis_index("dp")
    c = lax.axis_index("tensor")
    c1, zc = c.reshape(1), jnp.stack([z, c])
    sent = prep(zc, tokens, ids.T, weights.T)
    came = []
    for j, piece in enumerate(sent):
        came.append(lax.ppermute(piece, ("dp", "tensor"), paired(-j, -j) if j else paired(0, 4)))
    packed, shared_own, ext = pack(*came)
    arrived = lax.all_to_all(packed, "expert", 0, 0, tiled=True)
    both = jnp.concatenate([arrived.reshape(4 * ROWS, BLOCK), shared_own])
    both = lax.ppermute(both, "tensor", SWAP)
    shared_oth = both[4 * ROWS :]
    own, oth = [
        jnp.moveaxis(a.reshape(EXPERTS, 4, CAP, BLOCK), 1, 0).reshape(4, ROWS, BLOCK)
        for a in (arrived, both[: 4 * ROWS])
    ]
    args = (c1, own, oth, shared_own, shared_oth, wg, wu, sg, su)
    early = up_dots(EARLY, *args)
    late = up_dots(LATE, *args)
    gate = dict(zip(EARLY + LATE, early[: len(EARLY)] + late[: len(LATE)]))
    up = dict(zip(EARLY + LATE, early[len(EARLY) :] + late[len(LATE) :]))
    g_down = ring([gate[k] for k in (4, 3, 2, 1)], -1)
    u_up = ring([up[k] for k in (4, 5, 6, 7)], 1)
    u_down = ring([up[k] for k in (3, 2, 1)], -1)
    g_up = ring([gate[k] for k in (5, 6, 7)], 1)
    g = (gate[0] + (g_down + g_up)) * (1.0 / SCALE)
    u = (up[0] + (u_down + u_up)) * (1.0 / SCALE)
    hidden = (jax.nn.silu(g) * u).astype(jnp.bfloat16)
    top, tail = hidden[:, :CUT], hidden[:, CUT:]
    got = {0: (top, tail)}
    pd, pu, qd, qu = top, top, tail, tail
    for j in range(1, 5):
        pd = lax.ppermute(pd, "dp", shifted(-1))
        qu = lax.ppermute(qu, "dp", shifted(1))
        if j < 4:
            qd = lax.ppermute(qd, "dp", shifted(-1))
            pu = lax.ppermute(pu, "dp", shifted(1))
            got[ZN - j], got[j] = (pd, qd), (pu, qu)
        else:
            got[4] = (pd, qu)
    keeps, sends = [], []
    for a, b in (((7, 6), (1, 2)), ((5, 0), (3, 4))):
        keep, send = down_dots(c1, [p for k in a + b for p in got[k]], wd, sd)
        keeps.append(keep)
        sends.append(send)
    crossed = lax.ppermute(jnp.concatenate(sends), "tensor", SWAP)
    rows, shared = settle(*keeps, crossed)
    back = lax.all_to_all(rows, "expert", 0, 0, tiled=True).reshape(4 * ROWS, BLOCK)
    mixed = combine(ext, back, shared)
    held = []
    for i, (to, fro) in enumerate(((1, 1), (2, 2), (3, 3), (0, 4))):
        held.append(lax.ppermute(mixed[i * PADT : (i + 1) * PADT], ("dp", "tensor"), paired(to, fro)))
    held = jnp.concatenate(held)
    others = lax.ppermute(held, "tensor", SWAP)
    return assemble(zc, held, others)


def solution(mesh):
    placed = (
        P(("dp", "expert"), None),
        P(("dp", "expert"), None),
        P(("dp", "expert"), None),
        P("expert", "dp", "tensor"),
        P("expert", "dp", "tensor"),
        P("expert", "tensor", "dp"),
        P("dp", "tensor"),
        P("dp", "tensor"),
        P("tensor", "dp"),
    )
    return jax.shard_map(layer, mesh=mesh, in_specs=placed, out_specs=P(("dp", "expert"), None), check_vma=False)
```

```python
import functools

import jax
import jax.numpy as jnp
from jax import lax
from jax.experimental import pallas as pl
from jax.experimental.pallas import tpu as pltpu
from jax.sharding import PartitionSpec as P

EXPERTS = 16
CAP = 8
TOP = 8
ZN = 8
TOK = 12
PADT = 16
BLOCK = 896
ROWS = EXPERTS * CAP
CHUNK = ROWS + PADT
FFH = 1024
CUT = FFH // 2
NT = 256
EXT = 128
HELD = ((0, 7, 6, 5), (4, 1, 2, 3))
EARLY = (3, 4, 5)
LATE = (6, 7, 0, 1, 2)
SCALE = 16.0
LINK = jnp.float16

PARAMS = pltpu.CompilerParams(vmem_limit_bytes=16 * 1024 * 1024)
VMEM = pl.BlockSpec(memory_space=pltpu.VMEM)
SMEM = pl.BlockSpec(memory_space=pltpu.SMEM)
SWAP = [(0, 1), (1, 0)]


def shifted(k):
    return [(i, (i + k) % ZN) for i in range(ZN)]


def paired(up, down):
    out = []
    for i in range(ZN):
        out.append((i * 2, ((i + up) % ZN) * 2))
        out.append((i * 2 + 1, ((i - down) % ZN) * 2 + 1))
    return out


def fdot(a, b):
    return jnp.dot(a, b, preferred_element_type=jnp.float32)


def prep_kernel(s_ref, x_hbm, ids_hbm, w_hbm, *refs):
    outs, (x_ref, ids_ref, w_ref, sems) = refs[:4], refs[4:]
    z, c = s_ref[0], s_ref[1]
    pairs = ((ids_hbm, ids_ref), (w_hbm, w_ref), (x_hbm, x_ref))
    copies = [pltpu.make_async_copy(a, b, sems.at[i]) for i, (a, b) in enumerate(pairs)]
    for copy in copies:
        copy.start()
    for copy in copies:
        copy.wait()
    w = w_ref[...]
    hi = w.astype(jnp.bfloat16)
    rest = w - hi.astype(jnp.float32)
    mid = rest.astype(jnp.bfloat16)
    low = (rest - mid.astype(jnp.float32)).astype(jnp.bfloat16)
    lane = lax.broadcasted_iota(jnp.int32, (TOP, EXT), 1)
    part = lax.broadcasted_iota(jnp.int32, (TOP, EXT), 0)
    ext = jnp.zeros((TOK, EXT), jnp.float32)
    for i, v in enumerate((ids_ref[...].astype(jnp.float32).astype(jnp.bfloat16), hi, mid, low)):
        spread = (lane == TOP * i + part).astype(jnp.bfloat16)
        ext = ext + lax.dot_general(v, spread, (((0,), (0,)), ((), ())), preferred_element_type=jnp.float32)
    ext = ext.astype(jnp.bfloat16)
    for j, out_ref in enumerate(outs):
        block = (z + 4 * c) % ZN if j == 0 else (z + ZN + jnp.where(c == 0, -j, j)) % ZN
        out_ref[...] = jnp.zeros((PADT, BLOCK + EXT), jnp.bfloat16)
        out_ref[:TOK, :BLOCK] = x_ref[:, pl.ds(pl.multiple_of(block * BLOCK, 128), BLOCK)]
        out_ref[:TOK, BLOCK:] = ext


def prep(s, x, ids, w):
    return pl.pallas_call(
        prep_kernel,
        out_shape=(jax.ShapeDtypeStruct((PADT, BLOCK + EXT), jnp.bfloat16),) * 4,
        in_specs=[SMEM] + [pl.BlockSpec(memory_space=pltpu.HBM)] * 3,
        out_specs=(VMEM,) * 4,
        scratch_shapes=[
            pltpu.VMEM((TOK, ZN * BLOCK), jnp.bfloat16),
            pltpu.VMEM((TOP, TOK), jnp.int32),
            pltpu.VMEM((TOP, TOK), jnp.float32),
            pltpu.SemaphoreType.DMA((3,)),
        ],
        compiler_params=PARAMS,
        name="prep",
    )(s, x, ids, w)


def pack_kernel(*refs):
    xs, (packed_ref, shared_ref, ext_ref) = refs[:4], refs[4:]
    n = 4 * PADT
    for i, x in enumerate(xs):
        shared_ref[i * PADT : (i + 1) * PADT] = x[:, :BLOCK]
        ext_ref[i * PADT : (i + 1) * PADT] = x[:, BLOCK:]
    x = shared_ref[...]
    ids = jnp.transpose(ext_ref[...].astype(jnp.float32))[:TOP, :].astype(jnp.int32)
    experts = lax.broadcasted_iota(jnp.int32, (EXPERTS, n), 0)
    row = lax.broadcasted_iota(jnp.int32, (EXPERTS, n), 1)
    member = jnp.zeros((EXPERTS, n), jnp.float32)
    for k in range(TOP):
        member = member + ((experts == ids[k : k + 1, :]) & (row % PADT < TOK)).astype(jnp.float32)
    r0 = lax.broadcasted_iota(jnp.int32, (n, n), 0)
    r1 = lax.broadcasted_iota(jnp.int32, (n, n), 1)
    before = ((r0 // PADT == r1 // PADT) & (r0 < r1)).astype(jnp.bfloat16)
    pos = fdot(member.astype(jnp.bfloat16), before).astype(jnp.int32)
    target = jnp.where(member > 0.5, row // PADT * CAP + pos, -1)
    wanted = lax.broadcasted_iota(jnp.int32, (4 * CAP, n), 0)
    for e in range(EXPERTS):
        pick = (wanted == target[e : e + 1, :]).astype(jnp.bfloat16)
        packed_ref[e] = fdot(pick, x).astype(jnp.bfloat16)


def pack(*xs):
    return pl.pallas_call(
        pack_kernel,
        out_shape=(
            jax.ShapeDtypeStruct((EXPERTS, 4 * CAP, BLOCK), jnp.bfloat16),
            jax.ShapeDtypeStruct((4 * PADT, BLOCK), jnp.bfloat16),
            jax.ShapeDtypeStruct((4 * PADT, EXT), jnp.bfloat16),
        ),
        in_specs=[VMEM] * 4,
        out_specs=(VMEM, VMEM, VMEM),
        compiler_params=PARAMS,
        name="pack",
    )(*xs)


def up_kernel(ks, c_ref, own_ref, oth_ref, so_ref, st_ref, wg_ref, wu_ref, sg_ref, su_ref, *refs):
    count = len(ks)
    out_refs, (x_ref, s_ref, full_ref) = refs[:-3], refs[-3:]

    def gather(sides):
        for at, k in enumerate(ks):
            side = 0 if k in HELD[0] else 1
            i = HELD[side].index(k)
            full, shared = sides[side]
            x_ref[at * ROWS : (at + 1) * ROWS] = full[i]
            s_ref[at * PADT : (at + 1) * PADT] = shared[i * PADT : (i + 1) * PADT]

    own, oth = (own_ref, so_ref), (oth_ref, st_ref)
    start = pl.program_id(0) == 0

    @pl.when(start & (c_ref[0] == 0))
    def _():
        gather((own, oth))

    @pl.when(start & (c_ref[0] != 0))
    def _():
        gather((oth, own))

    for w_ref, v_ref, o_refs in ((wg_ref, sg_ref, out_refs[:count]), (wu_ref, su_ref, out_refs[count:])):
        shared = fdot(s_ref[...], v_ref[...]) * SCALE
        full_ref[...] = fdot(x_ref[...], w_ref[0]) * SCALE
        for i in range(count):
            o_refs[i][:ROWS, :] = full_ref[i * ROWS : (i + 1) * ROWS]
            o_refs[i][ROWS:, :] = shared[i * PADT : (i + 1) * PADT]


def up_dots(ks, c, own, oth, so, st, wg, wu, sg, su):
    whole = lambda *shape: pl.BlockSpec(shape, lambda n: (0,) * len(shape))
    count = len(ks)
    return pl.pallas_call(
        functools.partial(up_kernel, ks),
        grid=(FFH // NT,),
        out_shape=(jax.ShapeDtypeStruct((CHUNK, FFH), jnp.float32),) * (2 * count),
        in_specs=[
            SMEM,
            whole(4, ROWS, BLOCK),
            whole(4, ROWS, BLOCK),
            whole(4 * PADT, BLOCK),
            whole(4 * PADT, BLOCK),
            pl.BlockSpec((1, BLOCK, NT), lambda n: (0, 0, n)),
            pl.BlockSpec((1, BLOCK, NT), lambda n: (0, 0, n)),
            pl.BlockSpec((BLOCK, NT), lambda n: (0, n)),
            pl.BlockSpec((BLOCK, NT), lambda n: (0, n)),
        ],
        out_specs=(pl.BlockSpec((CHUNK, NT), lambda n: (0, n)),) * (2 * count),
        scratch_shapes=[
            pltpu.VMEM((count * ROWS, BLOCK), jnp.bfloat16),
            pltpu.VMEM((count * PADT, BLOCK), jnp.bfloat16),
            pltpu.VMEM((count * ROWS, NT), jnp.float32),
        ],
        compiler_params=PARAMS,
        cost_estimate=pl.CostEstimate(
            flops=2 * 2 * count * CHUNK * BLOCK * FFH, bytes_accessed=4 * BLOCK * FFH * 2, transcendentals=0
        ),
    )(c, own, oth, so, st, wg, wu, sg, su)


def down_kernel(c_ref, *refs):
    xs, (wd_ref, sd_ref, keep_ref, send_ref, x_ref, s_ref, full_ref) = refs[:-7], refs[-7:]
    n = len(xs) // 4
    for i in range(2 * n):
        for x, cols in zip(xs[2 * i : 2 * i + 2], (slice(0, CUT), slice(CUT, FFH))):
            x_ref[i, :, cols] = x[:ROWS]
            s_ref[i * PADT : (i + 1) * PADT, cols] = x[ROWS:]

    def chunk(i, carry):
        full_ref[i, :ROWS] = fdot(x_ref[i], wd_ref[0])
        return carry

    lax.fori_loop(0, 2 * n, chunk, 0)
    shared = fdot(s_ref[...], sd_ref[...])
    for i in range(2 * n):
        full_ref[i, ROWS:] = shared[i * PADT : (i + 1) * PADT]
    c = c_ref[0]
    for i in range(n):
        keep_ref[i] = full_ref[c * n + i]
        send_ref[i] = full_ref[(1 - c) * n + i].astype(jnp.bfloat16)


def down_dots(c, xs, wd, sd):
    n = len(xs) // 4
    return pl.pallas_call(
        down_kernel,
        out_shape=(
            jax.ShapeDtypeStruct((n, CHUNK, BLOCK), jnp.float32),
            jax.ShapeDtypeStruct((n, CHUNK, BLOCK), jnp.bfloat16),
        ),
        in_specs=[SMEM] + [VMEM] * (len(xs) + 2),
        out_specs=(VMEM, VMEM),
        scratch_shapes=[
            pltpu.VMEM((2 * n, ROWS, FFH), jnp.bfloat16),
            pltpu.VMEM((2 * n * PADT, FFH), jnp.bfloat16),
            pltpu.VMEM((2 * n, CHUNK, BLOCK), jnp.float32),
        ],
        compiler_params=PARAMS,
        cost_estimate=pl.CostEstimate(
            flops=2 * 2 * n * CHUNK * BLOCK * FFH, bytes_accessed=2 * BLOCK * FFH * 2, transcendentals=0
        ),
        name="down_dots",
    )(c, *xs, wd, sd)


def settle_kernel(near_ref, far_ref, came_ref, rows_ref, shared_ref):
    for i in range(4):
        keep = (near_ref, far_ref)[i // 2]
        total = keep[i % 2, :ROWS] + came_ref[i, :ROWS].astype(jnp.float32)
        rows_ref[:, i * CAP : (i + 1) * CAP, :] = total.reshape(EXPERTS, CAP, BLOCK).astype(jnp.bfloat16)
        shared_ref[i * PADT : (i + 1) * PADT] = keep[i % 2, ROWS:] + came_ref[i, ROWS:].astype(jnp.float32)


def settle(near, far, came):
    return pl.pallas_call(
        settle_kernel,
        out_shape=(
            jax.ShapeDtypeStruct((EXPERTS, 4 * CAP, BLOCK), jnp.bfloat16),
            jax.ShapeDtypeStruct((4 * PADT, BLOCK), jnp.float32),
        ),
        in_specs=[VMEM] * 3,
        out_specs=(VMEM, VMEM),
        compiler_params=PARAMS,
        name="settle",
    )(near, far, came)


def terms_kernel(ext_ref, terms_ref):
    rows = 4 * PADT
    cols = 4 * ROWS
    ext = jnp.concatenate([ext_ref[PADT:], ext_ref[:PADT]], axis=0).astype(jnp.float32)
    weight = (ext[:, TOP : 2 * TOP] + ext[:, 2 * TOP : 3 * TOP]) + ext[:, 3 * TOP : 4 * TOP]
    column = lax.broadcasted_iota(jnp.int32, (rows, cols), 1)
    row = lax.broadcasted_iota(jnp.int32, (rows, cols), 0)
    live = (row % PADT < TOK) & (row // PADT == (column // CAP) % 4)
    owner = (column // (4 * CAP)).astype(jnp.float32)
    slot = (column % CAP).astype(jnp.float32)
    member = jnp.zeros((rows, cols), jnp.float32)
    scale = jnp.zeros((rows, cols), jnp.float32)
    for k in range(TOP):
        hit = (ext[:, k : k + 1] == owner) & live
        member = jnp.where(hit, 1.0, member)
        scale = jnp.where(hit, weight[:, k : k + 1], scale)
    i0 = lax.broadcasted_iota(jnp.int32, (rows, rows), 0)
    i1 = lax.broadcasted_iota(jnp.int32, (rows, rows), 1)
    before = ((i1 < i0) & (i0 // PADT == i1 // PADT)).astype(jnp.bfloat16)
    pos = fdot(before, member.astype(jnp.bfloat16))
    scale = jnp.where((pos == slot) & (member > 0.5), scale, 0.0)
    hi = scale.astype(jnp.bfloat16)
    rest = scale - hi.astype(jnp.float32)
    mid = rest.astype(jnp.bfloat16)
    low = (rest - mid.astype(jnp.float32)).astype(jnp.bfloat16)
    for i, term in enumerate((low, mid, hi)):
        terms_ref[i] = term


def terms(ext):
    return pl.pallas_call(
        terms_kernel,
        out_shape=jax.ShapeDtypeStruct((3, 4 * PADT, 4 * ROWS), jnp.bfloat16),
        in_specs=[VMEM],
        out_specs=VMEM,
        compiler_params=PARAMS,
        name="terms",
    )(ext)


def combine_kernel(terms_ref, back_ref, shared_ref, out_ref, total_ref):
    total_ref[...] = shared_ref[...]

    def add(i, carry):
        total_ref[...] += fdot(terms_ref[i], back_ref[...])
        return carry

    lax.fori_loop(0, 3, add, 0)
    out_ref[...] = total_ref[...].astype(jnp.bfloat16)


def combine(scales, back, shared):
    return pl.pallas_call(
        combine_kernel,
        out_shape=jax.ShapeDtypeStruct((4 * PADT, BLOCK), jnp.bfloat16),
        in_specs=[VMEM, VMEM, VMEM],
        out_specs=VMEM,
        scratch_shapes=[
            pltpu.VMEM((4 * PADT, BLOCK), jnp.float32),
        ],
        compiler_params=PARAMS,
        name="combine",
    )(scales, back, shared)


def assemble_kernel(s_ref, *refs):
    out_ref = refs[-1]
    z = s_ref[0]
    held_ref, came_ref = refs[:-1]
    a1, a2, b3, b0 = [held_ref[i * PADT : i * PADT + TOK] for i in range(4)]
    o1, o2, o3, o0 = [came_ref[i * PADT : i * PADT + TOK] for i in range(4)]

    def put(parts):
        for i, part in enumerate(parts):
            at = pl.multiple_of(((z + i) % ZN) * BLOCK, 128)
            out_ref[:, pl.ds(at, BLOCK)] = part

    @pl.when(s_ref[1] == 0)
    def _():
        put((b0, o1, o2, o3, o0, b3, a2, a1))

    @pl.when(s_ref[1] != 0)
    def _():
        put((o0, a1, a2, b3, b0, o3, o2, o1))


def assemble(s, *parts):
    return pl.pallas_call(
        assemble_kernel,
        out_shape=jax.ShapeDtypeStruct((TOK, ZN * BLOCK), jnp.bfloat16),
        in_specs=[SMEM] + [VMEM] * len(parts),
        out_specs=VMEM,
        compiler_params=PARAMS,
        name="assemble",
    )(s, *parts)


def ring(parts, shift):
    total = None
    for mine in parts:
        total = mine if total is None else mine + total.astype(jnp.float32)
        total = lax.ppermute(total.astype(LINK), "dp", shifted(shift))
    return total.astype(jnp.float32)


def layer(tokens, ids, weights, wg, wu, wd, sg, su, sd):
    z = lax.axis_index("dp")
    c = lax.axis_index("tensor")
    c1, zc = c.reshape(1), jnp.stack([z, c])
    held_out = [pltpu.with_memory_space_constraint(a, pltpu.HBM) for a in (tokens, ids.T, weights.T)]
    sent = prep(zc, *held_out)
    came = []
    for j, piece in enumerate(sent):
        came.append(lax.ppermute(piece, ("dp", "tensor"), paired(-j, -j) if j else paired(0, 4)))
    packed, shared_own, ext = pack(*came)
    arrived = lax.all_to_all(packed, "expert", 0, 0, tiled=True)
    both = jnp.concatenate([arrived.reshape(4 * ROWS, BLOCK), shared_own])
    both = lax.ppermute(both, "tensor", SWAP)
    shared_oth = both[4 * ROWS :]
    own, oth = [
        jnp.moveaxis(a.reshape(EXPERTS, 4, CAP, BLOCK), 1, 0).reshape(4, ROWS, BLOCK)
        for a in (arrived, both[: 4 * ROWS])
    ]
    args = (c1, own, oth, shared_own, shared_oth, wg, wu, sg, su)
    early = up_dots(EARLY, *args)
    late = up_dots(LATE, *args)
    gate = dict(zip(EARLY + LATE, early[: len(EARLY)] + late[: len(LATE)]))
    up = dict(zip(EARLY + LATE, early[len(EARLY) :] + late[len(LATE) :]))
    g_down = ring([gate[k] for k in (4, 3, 2, 1)], -1)
    u_up = ring([up[k] for k in (4, 5, 6, 7)], 1)
    u_down = ring([up[k] for k in (3, 2, 1)], -1)
    g_up = ring([gate[k] for k in (5, 6, 7)], 1)
    g = (gate[0] + (g_down + g_up)) * (1.0 / SCALE)
    u = (up[0] + (u_down + u_up)) * (1.0 / SCALE)
    hidden = (jax.nn.silu(g) * u).astype(jnp.bfloat16)
    top, tail = hidden[:, :CUT], hidden[:, CUT:]
    got = {0: (top, tail)}
    pd, pu, qd, qu = top, top, tail, tail
    for j in range(1, 5):
        pd = lax.ppermute(pd, "dp", shifted(-1))
        qu = lax.ppermute(qu, "dp", shifted(1))
        if j < 4:
            qd = lax.ppermute(qd, "dp", shifted(-1))
            pu = lax.ppermute(pu, "dp", shifted(1))
            got[ZN - j], got[j] = (pd, qd), (pu, qu)
        else:
            got[4] = (pd, qu)
    scales = terms(ext)
    keeps, sends = [], []
    for a, b in (((7, 6), (1, 2)), ((5, 0), (3, 4))):
        keep, send = down_dots(c1, [p for k in a + b for p in got[k]], wd, sd)
        keeps.append(keep)
        sends.append(send)
    crossed = lax.ppermute(jnp.concatenate(sends), "tensor", SWAP)
    rows, shared = settle(*keeps, crossed)
    back = lax.all_to_all(rows, "expert", 0, 0, tiled=True).reshape(4 * ROWS, BLOCK)
    mixed = combine(scales, back, shared)
    held = []
    for i, (to, fro) in enumerate(((1, 1), (2, 2), (3, 3), (0, 4))):
        held.append(lax.ppermute(mixed[i * PADT : (i + 1) * PADT], ("dp", "tensor"), paired(to, fro)))
    held = jnp.concatenate(held)
    others = lax.ppermute(held, "tensor", SWAP)
    return assemble(zc, held, others)


def solution(mesh):
    placed = (
        P(("dp", "expert"), None),
        P(("dp", "expert"), None),
        P(("dp", "expert"), None),
        P("expert", "dp", "tensor"),
        P("expert", "dp", "tensor"),
        P("expert", "tensor", "dp"),
        P("dp", "tensor"),
        P("dp", "tensor"),
        P("tensor", "dp"),
    )
    return jax.shard_map(layer, mesh=mesh, in_specs=placed, out_specs=P(("dp", "expert"), None), check_vma=False)
```
